256 devices in a mesh: groups: 2 (over z), ha: 128 (over y, x, core).
Axes of the slice: x: 8, y: 8, z: 2, core: 2. Of those that a mesh axis runs over, the one named last changes fastest.
The devices are a block of a 8x8x16 slice.
Arguments:
- video: bfloat16 [8, 512, 256, 128], P('groups', 'ha'), parts along dimension 0, may hold values from -90 to 90
- cache_video: bfloat16 [4, 512, 256, 128], P('groups', 'ha'), parts along dimension 0, may hold values from -90 to 90
- cache_hidden: bfloat16 [4, 256, 128, 256], P('groups', 'ha'), parts along dimension 0, may hold values from -0.25 to 2
- kernel_down: bfloat16 [3, 3, 3, 128, 256], replicated, may hold values from -0.05103104 to 0.05103104
- gain_down: float32 [256], replicated, may hold values from 0.1 to 1.9
- shift_down: float32 [256], replicated, may hold values from -3 to 3
- kernel_mix: bfloat16 [3, 3, 3, 256, 256], replicated, may hold values from -0.03608439 to 0.03608439
- gain_mix: float32 [256], replicated, may hold values from 0.1 to 1.9
- shift_mix: float32 [256], replicated, may hold values from -3 to 3
Outputs:
- encoded: bfloat16 [8, 256, 128, 256], P('groups', 'ha'), parts along dimension 0
- next_cache: bfloat16 [4, 256, 128, 256], P('groups', 'ha'), parts along dimension 0
The draws below stay inside these ranges and needn't reach their ends.
There are 2 independent parts, one for each index of `groups`. The reference program is written for one: setup_inputs(seed, part) draws one part's arguments, and reference() takes and returns one part's arrays. A program takes and returns all parts, laid end to end along the dimension named above; an argument that names none is the same for every part. Nothing has to cross between parts.
All inputs are finite; a program needn't handle non-finite values.
Results may differ from the reference program's by a relative error of at most 0.0032.
Values may be sent and summed in bfloat16 or wider, within the bound.
No kernel may reach another device: no remote copies, remote signals or barrier semaphores. Data moves between devices by JAX's collectives and lax.ppermute only.
A program may use at most 64 MiB of HBM per device.

```python
import math
import jax
import jax.numpy as jnp
from jax import lax

C_IN = 128
C_OUT = 256
GROUPS = 32
FRAMES = 4
WIDTH = 256
HEIGHT = 512


def rough_noise(key, shape):
    return jnp.clip(jax.random.normal(key, shape, jnp.float32), -6.0, 6.0)


def scale_profiles(key):
    keys = jax.random.split(jax.random.fold_in(key, 7), 2)
    rising = jnp.exp(math.log(3.0) * jnp.arange(HEIGHT, dtype=jnp.float32) / HEIGHT)
    rowwise = rising * jnp.exp(jax.random.uniform(keys[0], (HEIGHT,), jnp.float32, 0.0, math.log(3.3)))
    columns = jnp.exp(jax.random.uniform(keys[1], (WIDTH,), jnp.float32, 0.0, math.log(10.0)))
    return (rowwise, columns)


def frames_field(key, own_key, frames):
    shared = rough_noise(jax.random.fold_in(key, 5), (1, HEIGHT, WIDTH, C_IN))
    own = rough_noise(own_key, (frames, HEIGHT, WIDTH, C_IN))
    base = 0.9 * shared + 0.44 * own
    rowwise, columns = scale_profiles(key)
    return 0.1 * base * rowwise[None, :, None, None] * columns[None, None, :, None]


def tap_kernel(key, fan_rows, fan_cols):
    keys = jax.random.split(key, 2)
    share = 0.25
    common = jax.random.normal(keys[0], (1, 1, 1, fan_rows, fan_cols), jnp.float32)
    taps = jax.random.normal(keys[1], (3, 3, 3, fan_rows, fan_cols), jnp.float32)
    limit = 0.99 * 3.0 / math.sqrt(27 * fan_rows)
    values = (math.sqrt(share) * common + math.sqrt(1.0 - share) * taps) / math.sqrt(27 * fan_rows)
    return jnp.clip(values, -limit, limit)


def draw_video(key, part):
    return frames_field(key, jax.random.fold_in(key, 11), FRAMES).astype(jnp.bfloat16)


def draw_cache_video(key, part):
    return frames_field(key, jax.random.fold_in(key, 23), 2).astype(jnp.bfloat16)


def draw_kernel_down(key, part):
    return tap_kernel(jax.random.fold_in(key, 31), C_IN, C_OUT).astype(jnp.bfloat16)


def draw_kernel_mix(key, part):
    return tap_kernel(jax.random.fold_in(key, 37), C_OUT, C_OUT).astype(jnp.bfloat16)


def block_levels(rng, extent, cuts, smallest, high):
    loudness = 1.0
    for dim, parts in cuts:
        heights = jax.random.uniform(jax.random.fold_in(jax.random.fold_in(rng, 6), dim), (parts,), jnp.float32, smallest / len(cuts), high / len(cuts))
        loudness = loudness * jnp.repeat(jnp.exp(heights), extent[dim] // parts).reshape((-1,) + (1,) * (len(extent) - 1 - dim))
    return loudness


def gaussian(rng, extent, scale, most, held_as=jnp.bfloat16):
    values = scale * jax.random.normal(rng, extent, jnp.float32)
    return jnp.clip(values, min=-most, max=most).astype(held_as)


def setup_inputs(seed: int = 0, part: int = 0) -> dict:
    splits = jax.random.split(jax.random.key(seed), 10)
    part_keys = jax.random.split(jax.random.fold_in(splits[9], part), 10)
    return {
        "video": draw_video(jax.random.fold_in(jax.random.fold_in(splits[9], part), 71), part),
        "cache_video": draw_cache_video(jax.random.fold_in(jax.random.fold_in(splits[9], part), 71), part),
        "cache_hidden": jnp.clip(-0.25 + 2.25 * jax.random.uniform(part_keys[2], (2, HEIGHT // 2, WIDTH // 2, C_OUT), jnp.float32) ** block_levels(part_keys[2], (2, HEIGHT // 2, WIDTH // 2, C_OUT), ((1, 128),), -0.2, 0.2), -0.25, 2.0).astype(jnp.bfloat16),
        "kernel_down": draw_kernel_down(jax.random.fold_in(splits[9], 71), part),
        "gain_down": jnp.clip(1.0 + 0.18 * jax.random.normal(splits[4], (C_OUT,), jnp.float32), 0.1, 1.9),
        "shift_down": gaussian(splits[5], (C_OUT,), 0.5, 3.0, jnp.float32),
        "kernel_mix": draw_kernel_mix(jax.random.fold_in(splits[9], 71), part),
        "gain_mix": jnp.clip(1.0 + 0.18 * jax.random.normal(splits[7], (C_OUT,), jnp.float32), 0.1, 1.9),
        "shift_mix": gaussian(splits[8], (C_OUT,), 0.5, 3.0, jnp.float32),
    }


def convolve(stack, kernel, strides):
    result = lax.conv_general_dilated(stack[None], kernel, strides, 'VALID', dimension_numbers=('NDHWC', 'DHWIO', 'NDHWC'), preferred_element_type=jnp.float32)
    return result[0]

def normalize(values, scales, offsets):
    per_group = values.shape[-1] // GROUPS
    members = values.shape[0] * values.shape[1] * values.shape[2] * per_group
    totals = lax.optimization_barrier(jnp.sum(values, axis=(0, 1, 2))).reshape(GROUPS, per_group).sum(1)
    center = jnp.repeat(totals / members, per_group)
    deviate = values - center
    squares = lax.optimization_barrier(jnp.sum(deviate * deviate, axis=(0, 1, 2))).reshape(GROUPS, per_group).sum(1)
    spread = jnp.repeat(squares / members, per_group)
    normed = deviate * lax.rsqrt(spread + 1e-06) * scales + offsets
    return jax.nn.silu(normed).astype(jnp.bfloat16)

def reference(video, cache_video, cache_hidden, kernel_down, gain_down, shift_down, kernel_mix, gain_mix, shift_mix):
    stacked = jnp.concatenate([cache_video, video], axis=0)
    stacked = jnp.pad(stacked, ((0, 0), (0, 1), (0, 1), (0, 0)))
    first = convolve(stacked, kernel_down, (1, 2, 2))
    hidden = normalize(first, gain_down, shift_down)
    padded = jnp.concatenate([cache_hidden, hidden], axis=0)
    padded = jnp.pad(padded, ((0, 0), (1, 1), (1, 1), (0, 0)))
    second = convolve(padded, kernel_mix, (1, 1, 1))
    encoded = normalize(second, gain_mix, shift_mix)
    return (encoded, hidden[FRAMES - 2:])
```

```python
import jax
import jax.numpy as jnp
from jax import lax
from jax.experimental import pallas as pl
from jax.experimental.pallas import tpu as pltpu
from jax.sharding import Mesh
from jax.sharding import PartitionSpec as P

GROUPS = 32
LANES = 128
EPS = 1e-6
HA = ("ha_0", "ha_1", "ha_2")
F32 = jnp.float32
BF16 = jnp.bfloat16
VMEM = pl.BlockSpec(memory_space=pltpu.VMEM)


def whole(shape, dtype):
    return jax.ShapeDtypeStruct(shape, dtype)


def group_onehot(channels, transpose):
    per_group = channels // GROUPS
    shape = (LANES, channels) if transpose else (channels, LANES)
    channel = lax.broadcasted_iota(jnp.int32, shape, 1 if transpose else 0)
    group = lax.broadcasted_iota(jnp.int32, shape, 0 if transpose else 1)
    return jnp.where(channel // per_group == group, 1.0, 0.0).astype(F32)


def exact_dot(a, b):
    return jnp.dot(a, b, precision=lax.Precision.HIGHEST, preferred_element_type=F32)


def local_moments(blocks, members):
    channels = blocks[0].shape[-1]
    onehot = group_onehot(channels, False)
    spread = group_onehot(channels, True)
    total = sum(jnp.sum(b, axis=0, keepdims=True) for b in blocks)
    sums = exact_dot(total, onehot)
    center = exact_dot(sums * (1.0 / members), spread)
    squares = sum(jnp.sum((b - center) * (b - center), axis=0, keepdims=True) for b in blocks)
    squares = exact_dot(squares, onehot)
    return sums + pltpu.roll(squares, GROUPS, 1)


def affine(stats, members, scales, offsets):
    count = stats.shape[0]
    sums = jnp.sum(stats, axis=0, keepdims=True)
    center = sums * (1.0 / (members * count))
    off = stats - members * center
    between = jnp.sum(off * off, axis=0, keepdims=True) * (1.0 / members)
    squares = pltpu.roll(sums, LANES - GROUPS, 1) + between
    spread = squares * (1.0 / (members * count))
    group = lax.broadcasted_iota(jnp.int32, spread.shape, 1) < GROUPS
    rate = jnp.where(group, lax.rsqrt(spread + EPS), 0.0)
    center = jnp.where(group, center, 0.0)
    expand = group_onehot(scales.shape[-1], True)
    return exact_dot(center, expand), exact_dot(rate, expand) * scales, offsets


def silu_norm(values, center, factor, offset):
    normed = (values - center) * factor + offset
    return normed / (1.0 + jnp.exp(-normed))


def down_kernel(cache_ref, video_ref, rim_ref, kernel_ref, first_ref, stats_ref, pairs_ref):
    frames, rows, width, c_in = video_ref.shape
    cached = cache_ref.shape[0]
    half = width // 2
    for f in range(cached + frames):
        for r in range(rows + 1):
            if r == rows:
                source = rim_ref.at[f, 0]
            elif f < cached:
                source = cache_ref.at[f, r]
            else:
                source = video_ref.at[f - cached, r]
            pairs_ref[f, r, :, :c_in] = source[pl.ds(0, half, stride=2), :]
            pairs_ref[f, r, :, c_in:] = source[pl.ds(1, half, stride=2), :]
    c_out = kernel_ref.shape[-1]
    last = lax.broadcasted_iota(jnp.int32, (half, c_out), 0) == half - 1
    both = jnp.concatenate([kernel_ref[a, b, c] for a in range(3) for b in range(3) for c in range(2)], axis=0)
    ahead = jnp.concatenate([kernel_ref[a, b, 2] for a in range(3) for b in range(3)], axis=0)
    blocks = []
    for i in range(rows // 2):
        taps = [
            pairs_ref[a : a + frames, 2 * i + b].reshape(frames * half, 2 * c_in)
            for a in range(3)
            for b in range(3)
        ]
        here = jnp.dot(jnp.concatenate(taps, axis=1), both, preferred_element_type=F32)
        next_ = jnp.dot(
            jnp.concatenate([t[:, :c_in] for t in taps], axis=1), ahead, preferred_element_type=F32
        )
        for t in range(frames):
            rolled = pltpu.roll(next_[t * half : (t + 1) * half], half - 1, 0)
            block = here[t * half : (t + 1) * half] + jnp.where(last, 0.0, rolled)
            first_ref[t, i] = block
    blocks = [first_ref[t, i] for t in range(frames) for i in range(rows // 2)]
    members = len(blocks) * half * (c_out // GROUPS)
    stats_ref[...] = local_moments(blocks, members)


def mix_kernel(
    first_ref, above_ref, below_ref, hidden_in_ref, cached_above_ref, cached_below_ref,
    stats_in_ref, gain_ref, shift_ref, edge_ref, kernel_ref,
    second_ref, next_ref, stats_ref, rows_ref,
):
    frames, rows, width, channels = first_ref.shape
    cached = hidden_in_ref.shape[0]
    members = frames * rows * width * (channels // GROUPS)
    center, factor, offset = affine(stats_in_ref[...], members, gain_ref[...], shift_ref[...])
    top = edge_ref[0, 0] > 0
    bottom = edge_ref[0, 1] > 0
    for f in range(cached):
        rows_ref[f, 0] = cached_above_ref[f, 0]
        rows_ref[f, rows + 1] = cached_below_ref[f, 0]
        for i in range(rows):
            rows_ref[f, 1 + i] = hidden_in_ref[f, i]
    for t in range(frames):
        for i in range(rows):
            hidden = silu_norm(first_ref[t, i], center, factor, offset).astype(BF16)
            rows_ref[cached + t, 1 + i] = hidden
            if t >= frames - 2:
                next_ref[t - (frames - 2), i] = hidden
        above = silu_norm(above_ref[t, 0], center, factor, offset)
        rows_ref[cached + t, 0] = jnp.where(top, 0.0, above).astype(BF16)
        below = silu_norm(below_ref[t, 0], center, factor, offset)
        rows_ref[cached + t, rows + 1] = jnp.where(bottom, 0.0, below).astype(BF16)
    weights = [
        jnp.concatenate([kernel_ref[a, b, c] for a in range(3) for b in range(3)], axis=0)
        for c in range(3)
    ]
    place = lax.broadcasted_iota(jnp.int32, (width, channels), 0)
    for i in range(rows):
        taps = jnp.concatenate(
            [
                rows_ref[a : a + frames, i + b].reshape(frames * width, channels)
                for a in range(3)
                for b in range(3)
            ],
            axis=1,
        )
        left, here, right = (jnp.dot(taps, w, preferred_element_type=F32) for w in weights)
        for t in range(frames):
            span = slice(t * width, (t + 1) * width)
            block = here[span] + jnp.where(place == 0, 0.0, pltpu.roll(left[span], 1, 0))
            block = block + jnp.where(place == width - 1, 0.0, pltpu.roll(right[span], width - 1, 0))
            second_ref[t, i] = block
    blocks = [second_ref[t, i] for t in range(frames) for i in range(rows)]
    stats_ref[...] = local_moments(blocks, members)


def final_kernel(second_ref, stats_ref, gain_ref, shift_ref, out_ref):
    frames, rows, width, channels = second_ref.shape
    members = frames * rows * width * (channels // GROUPS)
    center, factor, offset = affine(stats_ref[...], members, gain_ref[...], shift_ref[...])
    for t in range(frames):
        for i in range(rows):
            out_ref[t, i] = silu_norm(second_ref[t, i], center, factor, offset).astype(BF16)


def chain_pairs(by):
    count = lax.axis_size(HA)
    return [(i, i + by) for i in range(count) if 0 <= i + by < count]


def everyone(stats):
    count = lax.axis_size(HA)
    spread = jnp.broadcast_to(stats[None], (count, *stats.shape))
    return lax.all_to_all(spread, HA, 0, 0).reshape(count, stats.shape[-1])


def local(video, cache_video, cache_hidden, kernel_down, gain_down, shift_down, kernel_mix, gain_mix, shift_mix):
    frames, rows, width, _ = video.shape
    c_out = kernel_down.shape[-1]
    half = width // 2
    down = chain_pairs(1)
    up = chain_pairs(-1)
    rim = lax.ppermute(jnp.concatenate([cache_video[:, :1], video[:, :1]], axis=0), HA, up)
    cached_above = lax.ppermute(cache_hidden[:, -1:], HA, down)
    cached_below = lax.ppermute(cache_hidden[:, :1], HA, up)
    first, stats = pl.pallas_call(
        down_kernel,
        name="down",
        out_shape=(whole((frames, rows // 2, half, c_out), F32), whole((1, LANES), F32)),
        in_specs=[VMEM] * 4,
        out_specs=(VMEM, VMEM),
        scratch_shapes=[pltpu.VMEM((frames + 2, rows + 1, half, 2 * video.shape[-1]), BF16)],
    )(cache_video, video, rim, kernel_down)
    above = lax.ppermute(first[:, -1:], HA, down)
    below = lax.ppermute(first[:, :1], HA, up)
    stats = everyone(stats)
    place = lax.axis_index(HA)
    edge = jnp.stack([place == 0, place == lax.axis_size(HA) - 1]).astype(jnp.int32)[None]
    second, next_cache, stats = pl.pallas_call(
        mix_kernel,
        name="mix",
        out_shape=(
            whole(first.shape, F32),
            whole((2, *first.shape[1:]), BF16),
            whole((1, LANES), F32),
        ),
        in_specs=[VMEM] * 9 + [pl.BlockSpec(memory_space=pltpu.SMEM), VMEM],
        out_specs=(VMEM, VMEM, VMEM),
        scratch_shapes=[pltpu.VMEM((frames + 2, rows // 2 + 2, half, c_out), BF16)],
    )(
        first, above, below, cache_hidden, cached_above, cached_below,
        stats, gain_down[None], shift_down[None], edge, kernel_mix,
    )
    stats = everyone(stats)
    encoded = pl.pallas_call(
        final_kernel,
        name="final",
        out_shape=whole(first.shape, BF16),
        in_specs=[VMEM] * 4,
        out_specs=VMEM,
    )(second, stats, gain_mix[None], shift_mix[None])
    return (encoded, next_cache)


def solution(mesh):
    split = Mesh(
        mesh.devices.reshape(mesh.shape["groups"], 8, 8, 2), ("groups", "ha_0", "ha_1", "ha_2")
    )
    strips = P("groups", HA, None, None)
    return jax.shard_map(
        local,
        mesh=split,
        in_specs=(strips, strips, strips, P(), P(), P(), P(), P(), P()),
        out_specs=(strips, strips),
        check_vma=False,
    )
```

```python
import jax
import jax.numpy as jnp
from jax import lax
from jax.experimental import pallas as pl
from jax.experimental.pallas import tpu as pltpu
from jax.sharding import Mesh
from jax.sharding import PartitionSpec as P

GROUPS = 32
LANES = 128
EPS = 1e-6
HA = ("ha_0", "ha_1", "ha_2")
F32 = jnp.float32
BF16 = jnp.bfloat16
AUTO = pl.BlockSpec()
ANY = pl.BlockSpec(memory_space=pl.ANY)
HBM = pl.BlockSpec(memory_space=pltpu.HBM)
SMEM = pl.BlockSpec(memory_space=pltpu.SMEM)
DMA = pltpu.SemaphoreType.DMA


def limit(mib):
    return pltpu.CompilerParams(vmem_limit_bytes=mib * 2**20)


def lanes_of(x):
    return lax.broadcasted_iota(jnp.int32, x.shape, x.ndim - 1)


def turn(x, by):
    return pltpu.roll(x, by % x.shape[-1], x.ndim - 1)


def group_sum(x):
    lane = lanes_of(x)
    step = 1
    while step < x.shape[-1] // GROUPS:
        x = x + jnp.where((lane & step) != 0, turn(x, step), turn(x, -step))
        step *= 2
    return x


def column_sum(block):
    return jnp.sum(block, axis=0, keepdims=True)


def moments_row(center, sums, squares, count):
    members = count * (center.shape[-1] // GROUPS)
    shift = group_sum(sums) * (1.0 / members)
    squares = group_sum(squares) - shift * shift * members
    mean = center + shift
    kind = lanes_of(mean[:, :LANES]) % 4
    low = jnp.where(kind == 0, mean[:, :LANES], squares[:, :LANES])
    high = jnp.where(kind == 2, mean[:, LANES:], squares[:, LANES:])
    return jnp.where(kind < 2, low, high)


def affine(rows, members, gain):
    devices = rows.shape[0]
    total = column_sum(rows)
    center = total * (1.0 / devices)
    off = rows - center
    between = column_sum(off * off) * members
    spread = (total + turn(between, 1)) * (1.0 / (members * devices))
    rate = lax.rsqrt(jnp.maximum(spread, 0.0) + EPS)
    kind = lanes_of(total) % 4

    def fill(value, at):
        value = jnp.where(kind == at, value, 0.0)
        value = value + turn(value, 1 if at % 2 == 0 else -1)
        return value + turn(value, 2 if at < 2 else -2)

    centers = jnp.concatenate([fill(center, 0), fill(center, 2)], axis=1)
    rates = jnp.concatenate([fill(rate, 1), fill(rate, 3)], axis=1)
    return centers, rates * gain


def silu_norm(values, center, factor, offset):
    normed = (values - center) * factor + offset
    return normed / (1.0 + jnp.exp(-normed))


def shift_back(x):
    rows = x.shape[0]
    place = lax.broadcasted_iota(jnp.int32, x.shape, 0)
    return jnp.where(place == rows - 1, 0.0, pltpu.roll(x, rows - 1, 0))


def shift_on(x):
    place = lax.broadcasted_iota(jnp.int32, x.shape, 0)
    return jnp.where(place == 0, 0.0, pltpu.roll(x, 1, 0))


def rim_kernel(cache_ref, video_ref, out_ref, sems):
    cached = cache_ref.shape[0]
    copies = [
        pltpu.make_async_copy(cache_ref.at[:, 0], out_ref.at[:cached], sems.at[0]),
        pltpu.make_async_copy(video_ref.at[:, 0], out_ref.at[cached:], sems.at[1]),
    ]
    for c in copies:
        c.start()
    for c in copies:
        c.wait()


def pair_up(source, target, c_in):
    half = target.shape[0]
    target[:, :c_in] = source[pl.ds(0, half, stride=2), :]
    target[:, c_in:] = source[pl.ds(1, half, stride=2), :]


def down_kernel(
    cache_ref, video_ref, kernel_ref,
    row_ref, part_ref, third_ref, center_ref, sums_ref,
    cache_buf, video_buf, kernel_buf, pairs_ref, sems,
):
    frames, rows, width, c_in = video_ref.shape
    cached = cache_ref.shape[0]
    half = width // 2
    c_out = kernel_ref.shape[-1]
    loads = [
        pltpu.make_async_copy(cache_ref, cache_buf, sems.at[0]),
        pltpu.make_async_copy(video_ref, video_buf, sems.at[1]),
        pltpu.make_async_copy(kernel_ref.at[:, :2], kernel_buf, sems.at[2]),
        pltpu.make_async_copy(kernel_ref.at[:, 2], third_ref, sems.at[3]),
    ]
    for c in loads:
        c.start()
    for f in range(cached + frames):
        if f == 0:
            loads[0].wait()
        if f == cached:
            loads[1].wait()
        for r in range(rows):
            source = cache_buf.at[f, r] if f < cached else video_buf.at[f - cached, r]
            pair_up(source, pairs_ref.at[f, r], c_in)
    loads[2].wait()
    loads[3].wait()

    def tap(a, b, c):
        return third_ref[a, c] if b == 2 else kernel_buf[a, b, c]

    for i, depth in ((0, 3), (1, 2)):
        where = [(a, b) for b in range(depth) for a in range(3)]
        taps = [pairs_ref[a : a + frames, 2 * i + b].reshape(frames * half, 2 * c_in) for a, b in where]
        both = jnp.concatenate([tap(a, b, c) for a, b in where for c in range(2)], axis=0)
        ahead = jnp.concatenate([tap(a, b, 2) for a, b in where], axis=0)
        here = jnp.dot(jnp.concatenate(taps, axis=1), both, preferred_element_type=F32)
        evens = jnp.concatenate([t[:, :c_in] for t in taps], axis=1)
        after = jnp.dot(evens, ahead, preferred_element_type=F32)
        for t in range(frames):
            span = slice(t * half, (t + 1) * half)
            block = here[span] + shift_back(after[span])
            if i == 0:
                row_ref[t] = block
            else:
                part_ref[t] = block
    total = sum(column_sum(row_ref[t]) for t in range(frames))
    center = group_sum(total) * (1.0 / (frames * half * (c_out // GROUPS)))
    center_ref[...] = center
    sums_ref[0:1] = total - center * (frames * half)
    sums_ref[1:2] = sum(column_sum((row_ref[t] - center) ** 2) for t in range(frames))


def rim_down_kernel(
    core_ref, rim_ref, third_ref, row_ref, part_ref, center_ref, sums_ref, hidden_ref,
    last_ref, edge_a_ref, edge_b_ref, message_ref,
    pairs_ref, sems,
):
    frames, half, c_out = row_ref.shape
    c_in = rim_ref.shape[-1]
    cached = hidden_ref.shape[0]
    core = core_ref[0]
    loads = [
        pltpu.make_async_copy(hidden_ref.at[:, 1 - core], edge_a_ref.at[:cached], sems.at[0]),
        pltpu.make_async_copy(hidden_ref.at[:, core], edge_b_ref.at[:cached], sems.at[1]),
    ]
    for c in loads:
        c.start()
    for f in range(rim_ref.shape[0]):
        pair_up(rim_ref.at[f], pairs_ref.at[f], c_in)
    taps = [pairs_ref[a : a + frames].reshape(frames * half, 2 * c_in) for a in range(3)]
    both = jnp.concatenate([third_ref[a, c] for a in range(3) for c in range(2)], axis=0)
    ahead = jnp.concatenate([third_ref[a, 2] for a in range(3)], axis=0)
    here = jnp.dot(jnp.concatenate(taps, axis=1), both, preferred_element_type=F32)
    evens = jnp.concatenate([t[:, :c_in] for t in taps], axis=1)
    after = jnp.dot(evens, ahead, preferred_element_type=F32)
    center = center_ref[...]
    sums, squares = sums_ref[0:1], sums_ref[1:2]
    upper = core == 0
    for t in range(frames):
        span = slice(t * half, (t + 1) * half)
        block = part_ref[t] + here[span] + shift_back(after[span])
        last_ref[t] = block
        off = block - center
        sums = sums + column_sum(off)
        squares = squares + column_sum(off * off)
        other = row_ref[t]
        for edge_ref, value in (
            (edge_a_ref, jnp.where(upper, block, other)),
            (edge_b_ref, jnp.where(upper, other, block)),
        ):
            coarse = value.astype(BF16)
            edge_ref[cached + t] = coarse
            edge_ref[cached + frames + t] = (value - coarse.astype(F32)).astype(BF16)
    message = moments_row(center, sums, squares, 2 * frames * half)
    message_ref[...] = jnp.broadcast_to(message[None], message_ref.shape)
    for c in loads:
        c.wait()


def mix_kernel(
    core_ref, row_ref, last_ref, edge_a_ref, edge_b_ref, stats_ref, gain_ref, shift_ref, hidden_ref, kernel_ref,
    second_ref, next_ref, message_ref,
    rows_ref, sem,
):
    frames, width, channels = row_ref.shape
    cached = hidden_ref.shape[0]
    rows = 2
    core, top, bottom = core_ref[0], core_ref[1], core_ref[2]
    for f in range(cached):
        for i in range(rows):
            rows_ref[f, 1 + i] = hidden_ref[f, i]
    count = rows * frames * width
    center, factor = affine(stats_ref[...][:, 0], count * (channels // GROUPS), gain_ref[...])
    offset = shift_ref[...]
    for edge_ref, at, missing in (
        (edge_a_ref, jnp.where(core == 0, rows + 1, 0), jnp.where(core == 0, bottom, top)),
        (edge_b_ref, jnp.where(core == 0, 0, rows + 1), jnp.where(core == 0, top, bottom)),
    ):
        for f in range(cached):
            rows_ref[f, at] = jnp.where(missing != 0, jnp.zeros_like(edge_ref[f]), edge_ref[f])
        for t in range(frames):
            value = edge_ref[cached + t].astype(F32) + edge_ref[cached + frames + t].astype(F32)
            hidden = silu_norm(value, center, factor, offset)
            rows_ref[cached + t, at] = jnp.where(missing != 0, 0.0, hidden).astype(BF16)
    for t in range(frames):
        rows_ref[cached + t, 1] = silu_norm(row_ref[t], center, factor, offset).astype(BF16)
        rows_ref[cached + t, 2] = silu_norm(last_ref[t], center, factor, offset).astype(BF16)
    store = pltpu.make_async_copy(
        rows_ref.at[cached + frames - 2 : cached + frames, 1 : 1 + rows], next_ref, sem
    )
    store.start()
    for c in (1, 0, 2):
        weights = jnp.concatenate([kernel_ref[a, b, c] for a in range(3) for b in range(3)], axis=0)
        for i in range(rows):
            taps = jnp.concatenate(
                [
                    rows_ref[a : a + frames, i + b].reshape(frames * width, channels)
                    for a in range(3)
                    for b in range(3)
                ],
                axis=1,
            )
            result = jnp.dot(taps, weights, preferred_element_type=F32)
            for t in range(frames):
                block = result[t * width : (t + 1) * width]
                if c != 1:
                    block = shift_on(block) if c == 0 else shift_back(block)
                    block = block + second_ref[t, i]
                second_ref[t, i] = block
    total = sum(column_sum(second_ref[t, 0]) for t in range(frames))
    center = group_sum(total) * (1.0 / (frames * width * (channels // GROUPS)))
    offs = [second_ref[t, i] - center for t in range(frames) for i in range(rows)]
    sums = sum(column_sum(off) for off in offs)
    squares = sum(column_sum(off * off) for off in offs)
    message = moments_row(center, sums, squares, count)
    message_ref[...] = jnp.broadcast_to(message[None], message_ref.shape)
    store.wait()


def final_kernel(second_ref, stats_ref, gain_ref, shift_ref, out_ref, buf, sems):
    frames, rows, width, channels = second_ref.shape
    members = frames * rows * width * (channels // GROUPS)
    center, factor = affine(stats_ref[...][:, 0], members, gain_ref[...])
    offset = shift_ref[...]
    stores = []
    for t in range(frames):
        for i in range(rows):
            buf[t, i] = silu_norm(second_ref[t, i], center, factor, offset).astype(BF16)
        stores.append(pltpu.make_async_copy(buf.at[t], out_ref.at[t], sems.at[t]))
        stores[-1].start()
    for c in stores:
        c.wait()


def everyone(message):
    return lax.all_to_all(message, HA, 0, 0)


def local(video, cache_video, cache_hidden, kernel_down, gain_down, shift_down, kernel_mix, gain_mix, shift_mix):
    frames, rows, width, c_in = video.shape
    cached = cache_video.shape[0]
    c_out = kernel_down.shape[-1]
    half = width // 2
    video, cache_video, kernel_down = (
        pltpu.with_memory_space_constraint(x, pltpu.HBM) for x in (video, cache_video, kernel_down)
    )
    devices = lax.axis_size(HA)
    place, core = lax.axis_index(HA), lax.axis_index(HA[-1])
    whole = jax.ShapeDtypeStruct
    spot = jnp.stack([core, place == 0, place == devices - 1]).astype(jnp.int32)
    rim = pl.pallas_call(
        rim_kernel,
        name="rim",
        out_shape=whole((cached + frames, width, c_in), BF16),
        in_specs=[HBM] * 2,
        out_specs=AUTO,
        scratch_shapes=[DMA((2,))],
        compiler_params=limit(4),
    )(cache_video, video)
    rim = lax.ppermute(rim, HA, [(i + 1, i) for i in range(devices - 1)])
    line = whole((frames, half, c_out), F32)
    row, part, third, center, sums = pl.pallas_call(
        down_kernel,
        name="down",
        out_shape=(
            line,
            line,
            whole((3, 3, c_in, c_out), BF16),
            whole((1, c_out), F32),
            whole((2, c_out), F32),
        ),
        in_specs=[HBM] * 3,
        out_specs=(AUTO,) * 5,
        scratch_shapes=[
            pltpu.VMEM(cache_video.shape, BF16),
            pltpu.VMEM(video.shape, BF16),
            pltpu.VMEM((3, 2, 3, c_in, c_out), BF16),
            pltpu.VMEM((cached + frames, rows, half, 2 * c_in), BF16),
            DMA((4,)),
        ],
        compiler_params=limit(24),
        cost_estimate=pl.CostEstimate(flops=2 * 10**9, bytes_accessed=4 * 10**6, transcendentals=0),
    )(cache_video, video, kernel_down)
    edge = whole((cached + 2 * frames, half, c_out), BF16)
    message = whole((devices, 1, LANES), F32)
    last, edge_a, edge_b, stats = pl.pallas_call(
        rim_down_kernel,
        name="rim_down",
        out_shape=(line, edge, edge, message),
        in_specs=[SMEM] + [AUTO] * 6 + [ANY],
        out_specs=(AUTO,) * 4,
        scratch_shapes=[pltpu.VMEM((cached + frames, half, 2 * c_in), BF16), DMA((2,))],
        compiler_params=limit(16),
    )(spot, rim, third, row, part, center, sums, cache_hidden)
    within = [(i, i ^ 1) for i in range(devices)]
    across = [(i, j) for i in range(1, devices - 1) for j in [i + 1 if i % 2 else i - 1]]
    edge_a = lax.ppermute(edge_a, HA, within)
    edge_b = lax.ppermute(edge_b, HA, across)
    stats = everyone(stats)
    second, next_cache, stats = pl.pallas_call(
        mix_kernel,
        name="mix",
        out_shape=(whole((frames, 2, half, c_out), F32), whole((2, 2, half, c_out), BF16), message),
        in_specs=[SMEM] + [AUTO] * 9,
        out_specs=(AUTO, ANY, AUTO),
        scratch_shapes=[
            pltpu.VMEM((cached + frames, 4, half, c_out), BF16),
            DMA(()),
        ],
        compiler_params=limit(28),
    )(spot, row, last, edge_a, edge_b, stats, gain_down[None], shift_down[None], cache_hidden, kernel_mix)
    stats = everyone(stats)
    encoded = pl.pallas_call(
        final_kernel,
        name="final",
        out_shape=whole((frames, 2, half, c_out), BF16),
        in_specs=[AUTO] * 4,
        out_specs=ANY,
        scratch_shapes=[pltpu.VMEM((frames, 2, half, c_out), BF16), DMA((frames,))],
        compiler_params=limit(8),
    )(second, stats, gain_mix[None], shift_mix[None])
    return (encoded, next_cache)


def solution(mesh):
    split = Mesh(
        mesh.devices.reshape(mesh.shape["groups"], 8, 8, 2), ("groups", "ha_0", "ha_1", "ha_2")
    )
    strips = P("groups", HA, None, None)
    return jax.shard_map(
        local,
        mesh=split,
        in_specs=(strips, strips, strips, P(), P(), P(), P(), P(), P()),
        out_specs=(strips, strips),
        check_vma=False,
    )
```

```python
import jax
import jax.numpy as jnp
from jax import lax
from jax.experimental import pallas as pl
from jax.experimental.pallas import tpu as pltpu
from jax.sharding import Mesh
from jax.sharding import PartitionSpec as P

GROUPS = 32
LANES = 128
EPS = 1e-6
HA = ("ha_0", "ha_1", "ha_2")
F32 = jnp.float32
BF16 = jnp.bfloat16
AUTO = pl.BlockSpec()
ANY = pl.BlockSpec(memory_space=pl.ANY)
HBM = pl.BlockSpec(memory_space=pltpu.HBM)
DMA = pltpu.SemaphoreType.DMA


def limit(mib):
    return pltpu.CompilerParams(vmem_limit_bytes=mib * 2**20)


def lanes_of(x):
    return lax.broadcasted_iota(jnp.int32, x.shape, x.ndim - 1)


def turn(x, by):
    return pltpu.roll(x, by % x.shape[-1], x.ndim - 1)


def group_sum(x):
    lane = lanes_of(x)
    step = 1
    while step < x.shape[-1] // GROUPS:
        x = x + jnp.where((lane & step) != 0, turn(x, step), turn(x, -step))
        step *= 2
    return x


def column_sum(block):
    return jnp.sum(block, axis=0, keepdims=True)


def moments_row(center, sums, squares, count):
    members = count * (center.shape[-1] // GROUPS)
    shift = group_sum(sums) * (1.0 / members)
    squares = group_sum(squares) - shift * shift * members
    mean = center + shift
    kind = lanes_of(mean[:, :LANES]) % 4
    low = jnp.where(kind == 0, mean[:, :LANES], squares[:, :LANES])
    high = jnp.where(kind == 2, mean[:, LANES:], squares[:, LANES:])
    return jnp.where(kind < 2, low, high)


def affine(rows, members, gain):
    devices = rows.shape[0]
    total = column_sum(rows)
    center = total * (1.0 / devices)
    off = rows - center
    between = column_sum(off * off) * members
    spread = (total + turn(between, 1)) * (1.0 / (members * devices))
    rate = lax.rsqrt(jnp.maximum(spread, 0.0) + EPS)
    kind = lanes_of(total) % 4

    def fill(value, at):
        value = jnp.where(kind == at, value, 0.0)
        value = value + turn(value, 1 if at % 2 == 0 else -1)
        return value + turn(value, 2 if at < 2 else -2)

    centers = jnp.concatenate([fill(center, 0), fill(center, 2)], axis=1)
    rates = jnp.concatenate([fill(rate, 1), fill(rate, 3)], axis=1)
    return centers, rates * gain


def silu_norm(values, center, factor, offset):
    normed = (values - center) * factor + offset
    return normed / (1.0 + jnp.exp(-normed))


def shift_back(x):
    rows = x.shape[0]
    place = lax.broadcasted_iota(jnp.int32, x.shape, 0)
    return jnp.where(place == rows - 1, 0.0, pltpu.roll(x, rows - 1, 0))


def shift_on(x):
    place = lax.broadcasted_iota(jnp.int32, x.shape, 0)
    return jnp.where(place == 0, 0.0, pltpu.roll(x, 1, 0))


def rim_kernel(cache_ref, video_ref, out_ref, sems):
    cached = cache_ref.shape[0]
    copies = [
        pltpu.make_async_copy(cache_ref.at[:, 0], out_ref.at[:cached], sems.at[0]),
        pltpu.make_async_copy(video_ref.at[:, 0], out_ref.at[cached:], sems.at[1]),
    ]
    for c in copies:
        c.start()
    for c in copies:
        c.wait()


def pair_up(source, target, c_in):
    half = target.shape[0]
    target[:, :c_in] = source[pl.ds(0, half, stride=2), :]
    target[:, c_in:] = source[pl.ds(1, half, stride=2), :]


def split_in_two(value):
    coarse = value.astype(BF16)
    return coarse, (value - coarse.astype(F32)).astype(BF16)


def down_kernel(
    cache_ref, video_ref, kernel_ref, hidden_ref,
    row_ref, part_ref, third_ref, center_ref, sums_ref, edge_ref,
    cache_buf, video_buf, kernel_buf, pairs_ref, sems,
):
    frames, rows, width, c_in = video_ref.shape
    cached = cache_ref.shape[0]
    half = width // 2
    c_out = kernel_ref.shape[-1]
    loads = [
        pltpu.make_async_copy(cache_ref, cache_buf, sems.at[0]),
        pltpu.make_async_copy(video_ref, video_buf, sems.at[1]),
        pltpu.make_async_copy(kernel_ref.at[:, :2], kernel_buf, sems.at[2]),
        pltpu.make_async_copy(kernel_ref.at[:, 2], third_ref, sems.at[3]),
    ]
    for c in loads:
        c.start()
    for f in range(cached + frames):
        if f == 0:
            loads[0].wait()
        if f == cached:
            loads[1].wait()
        for r in range(rows):
            source = cache_buf.at[f, r] if f < cached else video_buf.at[f - cached, r]
            pair_up(source, pairs_ref.at[f, r], c_in)
    for f in range(cached):
        edge_ref[f] = hidden_ref[f, 0]
    loads[2].wait()
    loads[3].wait()

    def tap(a, b, c):
        return third_ref[a, c] if b == 2 else kernel_buf[a, b, c]

    for i, depth in ((0, 3), (1, 2)):
        where = [(a, b) for b in range(depth) for a in range(3)]
        taps = [pairs_ref[a : a + frames, 2 * i + b].reshape(frames * half, 2 * c_in) for a, b in where]
        both = jnp.concatenate([tap(a, b, c) for a, b in where for c in range(2)], axis=0)
        ahead = jnp.concatenate([tap(a, b, 2) for a, b in where], axis=0)
        here = jnp.dot(jnp.concatenate(taps, axis=1), both, preferred_element_type=F32)
        evens = jnp.concatenate([t[:, :c_in] for t in taps], axis=1)
        after = jnp.dot(evens, ahead, preferred_element_type=F32)
        for t in range(frames):
            span = slice(t * half, (t + 1) * half)
            block = here[span] + shift_back(after[span])
            if i == 0:
                row_ref[t] = block
                edge_ref[cached + t], edge_ref[cached + frames + t] = split_in_two(block)
            else:
                part_ref[t] = block
    total = sum(column_sum(row_ref[t]) for t in range(frames))
    center = group_sum(total) * (1.0 / (frames * half * (c_out // GROUPS)))
    center_ref[...] = center
    sums_ref[0:1] = total - center * (frames * half)
    sums_ref[1:2] = sum(column_sum((row_ref[t] - center) ** 2) for t in range(frames))


def rim_down_kernel(
    rim_ref, third_ref, part_ref, center_ref, sums_ref, hidden_ref,
    last_ref, edge_ref, message_ref,
    pairs_ref,
):
    frames, half, c_out = part_ref.shape
    c_in = rim_ref.shape[-1]
    cached, rows = hidden_ref.shape[:2]
    for f in range(rim_ref.shape[0]):
        pair_up(rim_ref.at[f], pairs_ref.at[f], c_in)
    for f in range(cached):
        edge_ref[f] = hidden_ref[f, rows - 1]
    taps = [pairs_ref[a : a + frames].reshape(frames * half, 2 * c_in) for a in range(3)]
    both = jnp.concatenate([third_ref[a, c] for a in range(3) for c in range(2)], axis=0)
    ahead = jnp.concatenate([third_ref[a, 2] for a in range(3)], axis=0)
    here = jnp.dot(jnp.concatenate(taps, axis=1), both, preferred_element_type=F32)
    evens = jnp.concatenate([t[:, :c_in] for t in taps], axis=1)
    after = jnp.dot(evens, ahead, preferred_element_type=F32)
    center = center_ref[...]
    sums, squares = sums_ref[0:1], sums_ref[1:2]
    for t in range(frames):
        span = slice(t * half, (t + 1) * half)
        block = part_ref[t] + here[span] + shift_back(after[span])
        last_ref[t] = block
        edge_ref[cached + t], edge_ref[cached + frames + t] = split_in_two(block)
        off = block - center
        sums = sums + column_sum(off)
        squares = squares + column_sum(off * off)
    message_ref[...] = moments_row(center, sums, squares, 2 * frames * half)


def unpack(stats_ref):
    both = stats_ref[...][:, 0]
    return jnp.concatenate([both[:, :LANES], both[:, LANES:]], axis=0)


def mix_kernel(
    row_ref, last_ref, above_ref, below_ref, ends_ref, stats_ref, gain_ref, shift_ref, hidden_ref, kernel_ref,
    second_ref, next_ref, message_ref,
    rows_ref, sem,
):
    frames, width, channels = row_ref.shape
    cached = hidden_ref.shape[0]
    rows = 2
    count = rows * frames * width
    for f in range(cached):
        rows_ref[f, 0] = above_ref[f]
        rows_ref[f, rows + 1] = below_ref[f]
        for i in range(rows):
            rows_ref[f, 1 + i] = hidden_ref[f, i]
    center, factor = affine(unpack(stats_ref), count * (channels // GROUPS), gain_ref[...])
    offset = shift_ref[...]
    keep_above, keep_below = ends_ref[0:1], ends_ref[1:2]

    def activate(t):
        for at, edge_ref, keep in ((0, above_ref, keep_above), (rows + 1, below_ref, keep_below)):
            value = edge_ref[cached + t].astype(F32) + edge_ref[cached + frames + t].astype(F32)
            hidden = silu_norm(value, center, factor, offset)
            rows_ref[cached + t, at] = jnp.where(keep > 0, hidden, 0.0).astype(BF16)
        rows_ref[cached + t, 1] = silu_norm(row_ref[t], center, factor, offset).astype(BF16)
        rows_ref[cached + t, 2] = silu_norm(last_ref[t], center, factor, offset).astype(BF16)

    weights = [
        jnp.concatenate([kernel_ref[a, b, c] for a in range(3) for b in range(3)], axis=0)
        for c in range(3)
    ]
    step = frames // 2
    for begin in range(0, frames, step):
        for t in range(begin, begin + step):
            activate(t)
        taps = jnp.concatenate(
            [
                rows_ref[begin + a : begin + a + step, b : b + rows].reshape(step * rows * width, channels)
                for a in range(3)
                for b in range(3)
            ],
            axis=1,
        )
        left, here, right = (jnp.dot(taps, w, preferred_element_type=F32) for w in weights)
        for n in range(step * rows):
            span = slice(n * width, (n + 1) * width)
            t, i = begin + n // rows, n % rows
            second_ref[t, i] = here[span] + shift_on(left[span]) + shift_back(right[span])
        if begin == 0:
            blocks = [second_ref[t, i] for t in range(step) for i in range(rows)]
            total = sum(column_sum(b) for b in blocks)
            middle = group_sum(total) * (2.0 / (count * (channels // GROUPS)))
    store = pltpu.make_async_copy(
        rows_ref.at[cached + frames - 2 : cached + frames, 1 : 1 + rows], next_ref, sem
    )
    store.start()
    offs = [second_ref[t, i] - middle for t in range(frames) for i in range(rows)]
    sums = sum(column_sum(off) for off in offs)
    squares = sum(column_sum(off * off) for off in offs)
    message_ref[...] = moments_row(middle, sums, squares, count)
    store.wait()


def final_kernel(second_ref, stats_ref, gain_ref, shift_ref, out_ref, buf, sems):
    frames, rows, width, channels = second_ref.shape
    members = frames * rows * width * (channels // GROUPS)
    center, factor = affine(unpack(stats_ref), members, gain_ref[...])
    offset = shift_ref[...]
    stores = []
    for t in range(frames):
        for i in range(rows):
            buf[t, i] = silu_norm(second_ref[t, i], center, factor, offset).astype(BF16)
        stores.append(pltpu.make_async_copy(buf.at[t], out_ref.at[t], sems.at[t]))
        stores[-1].start()
    for c in stores:
        c.wait()


def both_kernel(mine_ref, other_ref, out_ref):
    both = jnp.concatenate([mine_ref[...], other_ref[...]], axis=1)
    out_ref[...] = jnp.broadcast_to(both[None], out_ref.shape)


def everyone(message):
    devices, chips = lax.axis_size(HA), lax.axis_size(HA[:-1])
    other = lax.ppermute(message, HA, [(i, i ^ 1) for i in range(devices)])
    copies = pl.pallas_call(
        both_kernel,
        name="both",
        out_shape=jax.ShapeDtypeStruct((chips, 1, 2 * LANES), F32),
        in_specs=[AUTO] * 2,
        out_specs=AUTO,
        compiler_params=limit(1),
    )(message, other)
    return lax.all_to_all(copies, HA[:-1], 0, 0)


def local(video, cache_video, cache_hidden, kernel_down, gain_down, shift_down, kernel_mix, gain_mix, shift_mix):
    frames, rows, width, c_in = video.shape
    cached = cache_video.shape[0]
    c_out = kernel_down.shape[-1]
    half = width // 2
    video, cache_video, kernel_down = (
        pltpu.with_memory_space_constraint(x, pltpu.HBM) for x in (video, cache_video, kernel_down)
    )
    devices = lax.axis_size(HA)
    place = lax.axis_index(HA)
    up = [(i + 1, i) for i in range(devices - 1)]
    down = [(i, i + 1) for i in range(devices - 1)]
    whole = jax.ShapeDtypeStruct
    rim = pl.pallas_call(
        rim_kernel,
        name="rim",
        out_shape=whole((cached + frames, width, c_in), BF16),
        in_specs=[HBM] * 2,
        out_specs=AUTO,
        scratch_shapes=[DMA((2,))],
        compiler_params=limit(4),
    )(cache_video, video)
    rim = lax.ppermute(rim, HA, up)
    ends = jnp.broadcast_to(
        jnp.stack([place > 0, place < devices - 1]).astype(F32)[:, None], (2, c_out)
    )
    cache_hidden, ends = lax.optimization_barrier((cache_hidden, ends))
    line = whole((frames, half, c_out), F32)
    edge = whole((cached + 2 * frames, half, c_out), BF16)
    message = whole((1, LANES), F32)
    row, part, third, center, sums, below = pl.pallas_call(
        down_kernel,
        name="down",
        out_shape=(
            line,
            line,
            whole((3, 3, c_in, c_out), BF16),
            whole((1, c_out), F32),
            whole((2, c_out), F32),
            edge,
        ),
        in_specs=[HBM] * 3 + [AUTO],
        out_specs=(AUTO,) * 6,
        scratch_shapes=[
            pltpu.VMEM(cache_video.shape, BF16),
            pltpu.VMEM(video.shape, BF16),
            pltpu.VMEM((3, 2, 3, c_in, c_out), BF16),
            pltpu.VMEM((cached + frames, rows, half, 2 * c_in), BF16),
            DMA((4,)),
        ],
        compiler_params=limit(24),
        cost_estimate=pl.CostEstimate(flops=2 * 10**9, bytes_accessed=4 * 10**6, transcendentals=0),
    )(cache_video, video, kernel_down, cache_hidden)
    below = lax.ppermute(below, HA, up)
    last, above, stats = pl.pallas_call(
        rim_down_kernel,
        name="rim_down",
        out_shape=(line, edge, message),
        in_specs=[AUTO] * 6,
        out_specs=(AUTO,) * 3,
        scratch_shapes=[pltpu.VMEM((cached + frames, half, 2 * c_in), BF16)],
        compiler_params=limit(16),
    )(rim, third, part, center, sums, cache_hidden)
    above = lax.ppermute(above, HA, down)
    stats = everyone(stats)
    second, next_cache, stats = pl.pallas_call(
        mix_kernel,
        name="mix",
        out_shape=(whole((frames, 2, half, c_out), F32), whole((2, 2, half, c_out), BF16), message),
        in_specs=[AUTO] * 10,
        out_specs=(AUTO, ANY, AUTO),
        scratch_shapes=[
            pltpu.VMEM((cached + frames, 4, half, c_out), BF16),
            DMA(()),
        ],
        compiler_params=limit(28),
    )(row, last, above, below, ends, stats, gain_down[None], shift_down[None], cache_hidden, kernel_mix)
    stats = everyone(stats)
    encoded = pl.pallas_call(
        final_kernel,
        name="final",
        out_shape=whole((frames, 2, half, c_out), BF16),
        in_specs=[AUTO] * 4,
        out_specs=ANY,
        scratch_shapes=[pltpu.VMEM((frames, 2, half, c_out), BF16), DMA((frames,))],
        compiler_params=limit(8),
    )(second, stats, gain_mix[None], shift_mix[None])
    return (encoded, next_cache)


def solution(mesh):
    split = Mesh(
        mesh.devices.reshape(mesh.shape["groups"], 8, 8, 2), ("groups", "ha_0", "ha_1", "ha_2")
    )
    strips = P("groups", HA, None, None)
    return jax.shard_map(
        local,
        mesh=split,
        in_specs=(strips, strips, strips, P(), P(), P(), P(), P(), P()),
        out_specs=(strips, strips),
        check_vma=False,
    )
```

```python
import jax
import jax.numpy as jnp
from jax import lax
from jax.experimental import pallas as pl
from jax.experimental.pallas import tpu as pltpu
from jax.sharding import Mesh
from jax.sharding import PartitionSpec as P

GROUPS = 32
LANES = 128
EPS = 1e-6
HA = ("ha_0", "ha_1", "ha_2")
F32 = jnp.float32
BF16 = jnp.bfloat16
AUTO = pl.BlockSpec()
ANY = pl.BlockSpec(memory_space=pl.ANY)
HBM = pl.BlockSpec(memory_space=pltpu.HBM)
DMA = pltpu.SemaphoreType.DMA


def limit(mib):
    return pltpu.CompilerParams(vmem_limit_bytes=mib * 2**20)


def lanes_of(x):
    return lax.broadcasted_iota(jnp.int32, x.shape, x.ndim - 1)


def turn(x, by):
    return pltpu.roll(x, by % x.shape[-1], x.ndim - 1)


def group_sum(x):
    lane = lanes_of(x)
    step = 1
    while step < x.shape[-1] // GROUPS:
        x = x + jnp.where((lane & step) != 0, turn(x, step), turn(x, -step))
        step *= 2
    return x


def column_sum(block):
    return jnp.sum(block, axis=0, keepdims=True)


def moments_row(center, sums, squares, count):
    members = count * (center.shape[-1] // GROUPS)
    shift = group_sum(sums) * (1.0 / members)
    squares = group_sum(squares) - shift * shift * members
    mean = center + shift
    kind = lanes_of(mean[:, :LANES]) % 4
    low = jnp.where(kind == 0, mean[:, :LANES], squares[:, :LANES])
    high = jnp.where(kind == 2, mean[:, LANES:], squares[:, LANES:])
    return jnp.where(kind < 2, low, high)


def affine(rows, members, gain):
    devices = rows.shape[0]
    total = column_sum(rows)
    center = total * (1.0 / devices)
    off = rows - center
    between = column_sum(off * off) * members
    spread = (total + turn(between, 1)) * (1.0 / (members * devices))
    rate = lax.rsqrt(jnp.maximum(spread, 0.0) + EPS)
    kind = lanes_of(total) % 4

    def fill(value, at):
        value = jnp.where(kind == at, value, 0.0)
        value = value + turn(value, 1 if at % 2 == 0 else -1)
        return value + turn(value, 2 if at < 2 else -2)

    centers = jnp.concatenate([fill(center, 0), fill(center, 2)], axis=1)
    rates = jnp.concatenate([fill(rate, 1), fill(rate, 3)], axis=1)
    return centers, rates * gain


def silu_norm(values, center, factor, offset):
    normed = (values - center) * factor + offset
    return normed / (1.0 + jnp.exp(-normed))


def shift_back(x):
    rows = x.shape[0]
    place = lax.broadcasted_iota(jnp.int32, x.shape, 0)
    return jnp.where(place == rows - 1, 0.0, pltpu.roll(x, rows - 1, 0))


def shift_on(x):
    place = lax.broadcasted_iota(jnp.int32, x.shape, 0)
    return jnp.where(place == 0, 0.0, pltpu.roll(x, 1, 0))


def rim_kernel(cache_ref, video_ref, out_ref, sems):
    cached = cache_ref.shape[0]
    copies = [
        pltpu.make_async_copy(cache_ref.at[:, 0], out_ref.at[:cached], sems.at[0]),
        pltpu.make_async_copy(video_ref.at[:, 0], out_ref.at[cached:], sems.at[1]),
    ]
    for c in copies:
        c.start()
    for c in copies:
        c.wait()


def pair_up(source, target, c_in):
    half = target.shape[0]
    target[:, :c_in] = source[pl.ds(0, half, stride=2), :]
    target[:, c_in:] = source[pl.ds(1, half, stride=2), :]


def split_in_two(value):
    coarse = value.astype(BF16)
    return coarse, (value - coarse.astype(F32)).astype(BF16)


def down_kernel(
    cache_ref, video_ref, kernel_ref, hidden_ref,
    row_ref, part_ref, third_ref, center_ref, sums_ref, edge_ref,
    cache_buf, video_buf, kernel_buf, pairs_ref, sems,
):
    frames, rows, width, c_in = video_ref.shape
    cached = cache_ref.shape[0]
    half = width // 2
    c_out = kernel_ref.shape[-1]
    loads = [
        pltpu.make_async_copy(cache_ref, cache_buf, sems.at[0]),
        pltpu.make_async_copy(video_ref, video_buf, sems.at[1]),
        pltpu.make_async_copy(kernel_ref.at[:, :2], kernel_buf, sems.at[2]),
        pltpu.make_async_copy(kernel_ref.at[:, 2], third_ref, sems.at[3]),
        pltpu.make_async_copy(hidden_ref.at[:, 0], edge_ref.at[:cached], sems.at[4]),
    ]
    for c in loads:
        c.start()
    for f in range(cached + frames):
        if f == 0:
            loads[0].wait()
        if f == cached:
            loads[1].wait()
        for r in range(rows):
            source = cache_buf.at[f, r] if f < cached else video_buf.at[f - cached, r]
            pair_up(source, pairs_ref.at[f, r], c_in)
    loads[2].wait()
    loads[3].wait()

    def tap(a, b, c):
        return third_ref[a, c] if b == 2 else kernel_buf[a, b, c]

    for i, depth in ((0, 3), (1, 2)):
        where = [(a, b) for b in range(depth) for a in range(3)]
        taps = [pairs_ref[a : a + frames, 2 * i + b].reshape(frames * half, 2 * c_in) for a, b in where]
        both = jnp.concatenate([tap(a, b, c) for a, b in where for c in range(2)], axis=0)
        ahead = jnp.concatenate([tap(a, b, 2) for a, b in where], axis=0)
        here = jnp.dot(jnp.concatenate(taps, axis=1), both, preferred_element_type=F32)
        evens = jnp.concatenate([t[:, :c_in] for t in taps], axis=1)
        after = jnp.dot(evens, ahead, preferred_element_type=F32)
        for t in range(frames):
            span = slice(t * half, (t + 1) * half)
            block = here[span] + shift_back(after[span])
            if i == 0:
                row_ref[t] = block
                edge_ref[cached + t], edge_ref[cached + frames + t] = split_in_two(block)
            else:
                part_ref[t] = block
    total = sum(column_sum(row_ref[t]) for t in range(frames))
    center = group_sum(total) * (1.0 / (frames * half * (c_out // GROUPS)))
    center_ref[...] = center
    sums_ref[0:1] = total - center * (frames * half)
    sums_ref[1:2] = sum(column_sum((row_ref[t] - center) ** 2) for t in range(frames))
    loads[4].wait()


def rim_down_kernel(
    rim_ref, third_ref, part_ref, center_ref, sums_ref, hidden_ref,
    last_ref, edge_ref, message_ref,
    pairs_ref, sem,
):
    frames, half, _ = part_ref.shape
    c_in = rim_ref.shape[-1]
    cached, rows = hidden_ref.shape[:2]
    load = pltpu.make_async_copy(hidden_ref.at[:, rows - 1], edge_ref.at[:cached], sem)
    load.start()
    for f in range(rim_ref.shape[0]):
        pair_up(rim_ref.at[f], pairs_ref.at[f], c_in)
    taps = [pairs_ref[a : a + frames].reshape(frames * half, 2 * c_in) for a in range(3)]
    both = jnp.concatenate([third_ref[a, c] for a in range(3) for c in range(2)], axis=0)
    ahead = jnp.concatenate([third_ref[a, 2] for a in range(3)], axis=0)
    here = jnp.dot(jnp.concatenate(taps, axis=1), both, preferred_element_type=F32)
    evens = jnp.concatenate([t[:, :c_in] for t in taps], axis=1)
    after = jnp.dot(evens, ahead, preferred_element_type=F32)
    center = center_ref[...]
    sums, squares = sums_ref[0:1], sums_ref[1:2]
    for t in range(frames):
        span = slice(t * half, (t + 1) * half)
        block = part_ref[t] + here[span] + shift_back(after[span])
        last_ref[t] = block
        edge_ref[cached + t], edge_ref[cached + frames + t] = split_in_two(block)
        off = block - center
        sums = sums + column_sum(off)
        squares = squares + column_sum(off * off)
    message_ref[...] = moments_row(center, sums, squares, 2 * frames * half)
    load.wait()


def unpack(stats_ref):
    both = stats_ref[...][:, 0]
    return jnp.concatenate([both[:, :LANES], both[:, LANES:]], axis=0)


def mix_kernel(
    row_ref, last_ref, above_ref, below_ref, ends_ref, stats_ref, gain_ref, shift_ref, hidden_ref, kernel_ref,
    second_ref, next_ref, message_ref,
    rows_ref, kernel_buf, sems,
):
    frames, width, channels = row_ref.shape
    cached = hidden_ref.shape[0]
    rows = 2
    count = rows * frames * width
    load = pltpu.make_async_copy(hidden_ref, rows_ref.at[:cached, 1 : 1 + rows], sems.at[0])
    load.start()
    fetches = [
        pltpu.make_async_copy(kernel_ref.at[:, :, c], kernel_buf.at[c], sems.at[2 + c]) for c in range(3)
    ]
    for f in fetches:
        f.start()
    for f in range(cached):
        rows_ref[f, 0] = above_ref[f]
        rows_ref[f, rows + 1] = below_ref[f]
    center, factor = affine(unpack(stats_ref), count * (channels // GROUPS), gain_ref[...])
    offset = shift_ref[...]
    keep_above, keep_below = ends_ref[0:1], ends_ref[1:2]

    def activate(t):
        for at, edge_ref, keep in ((0, above_ref, keep_above), (rows + 1, below_ref, keep_below)):
            value = edge_ref[cached + t].astype(F32) + edge_ref[cached + frames + t].astype(F32)
            hidden = silu_norm(value, center, factor, offset)
            rows_ref[cached + t, at] = jnp.where(keep > 0, hidden, 0.0).astype(BF16)
        rows_ref[cached + t, 1] = silu_norm(row_ref[t], center, factor, offset).astype(BF16)
        rows_ref[cached + t, 2] = silu_norm(last_ref[t], center, factor, offset).astype(BF16)

    step = frames // 2
    for begin in range(0, frames, step):
        for t in range(begin, begin + step):
            activate(t)
        if begin == 0:
            load.wait()
        taps = jnp.concatenate(
            [
                rows_ref[begin + a : begin + a + step, b : b + rows].reshape(step * rows * width, channels)
                for a in range(3)
                for b in range(3)
            ],
            axis=1,
        )
        parts = []
        for c in range(3):
            if begin == 0:
                fetches[c].wait()
            weights = jnp.concatenate([kernel_buf[c, a, b] for a in range(3) for b in range(3)], axis=0)
            parts.append(jnp.dot(taps, weights, preferred_element_type=F32))
        left, here, right = parts
        for n in range(step * rows):
            span = slice(n * width, (n + 1) * width)
            t, i = begin + n // rows, n % rows
            second_ref[t, i] = here[span] + shift_on(left[span]) + shift_back(right[span])
        if begin == 0:
            blocks = [second_ref[t, i] for t in range(step) for i in range(rows)]
            total = sum(column_sum(b) for b in blocks)
            middle = group_sum(total) * (2.0 / (count * (channels // GROUPS)))
    store = pltpu.make_async_copy(
        rows_ref.at[cached + frames - 2 : cached + frames, 1 : 1 + rows], next_ref, sems.at[1]
    )
    store.start()
    offs = [second_ref[t, i] - middle for t in range(frames) for i in range(rows)]
    sums = sum(column_sum(off) for off in offs)
    squares = sum(column_sum(off * off) for off in offs)
    message_ref[...] = moments_row(middle, sums, squares, count)
    store.wait()


def final_kernel(second_ref, stats_ref, gain_ref, shift_ref, out_ref, buf, sems):
    frames, rows, width, channels = second_ref.shape
    members = frames * rows * width * (channels // GROUPS)
    center, factor = affine(unpack(stats_ref), members, gain_ref[...])
    offset = shift_ref[...]
    stores = []
    for t in range(frames):
        for i in range(rows):
            buf[t, i] = silu_norm(second_ref[t, i], center, factor, offset).astype(BF16)
        stores.append(pltpu.make_async_copy(buf.at[t], out_ref.at[t], sems.at[t]))
        stores[-1].start()
    for c in stores:
        c.wait()


def both_kernel(mine_ref, other_ref, out_ref):
    both = jnp.concatenate([mine_ref[...], other_ref[...]], axis=1)
    out_ref[...] = jnp.broadcast_to(both[None], out_ref.shape)


def everyone(message):
    devices, chips = lax.axis_size(HA), lax.axis_size(HA[:-1])
    other = lax.ppermute(message, HA, [(i, i ^ 1) for i in range(devices)])
    copies = pl.pallas_call(
        both_kernel,
        name="both",
        out_shape=jax.ShapeDtypeStruct((chips, 1, 2 * LANES), F32),
        in_specs=[AUTO] * 2,
        out_specs=AUTO,
        compiler_params=limit(1),
    )(message, other)
    return lax.all_to_all(copies, HA[:-1], 0, 0)


def local(video, cache_video, cache_hidden, kernel_down, gain_down, shift_down, kernel_mix, gain_mix, shift_mix):
    frames, rows, width, c_in = video.shape
    cached = cache_video.shape[0]
    c_out = kernel_down.shape[-1]
    half = width // 2
    video, cache_video, cache_hidden, kernel_mix = (
        pltpu.with_memory_space_constraint(x, pltpu.HBM)
        for x in (video, cache_video, cache_hidden, kernel_mix)
    )
    devices = lax.axis_size(HA)
    place = lax.axis_index(HA)
    up = [(i + 1, i) for i in range(devices - 1)]
    down = [(i, i + 1) for i in range(devices - 1)]
    whole = jax.ShapeDtypeStruct
    rim = pl.pallas_call(
        rim_kernel,
        name="rim",
        out_shape=whole((cached + frames, width, c_in), BF16),
        in_specs=[HBM] * 2,
        out_specs=AUTO,
        scratch_shapes=[DMA((2,))],
        compiler_params=limit(4),
    )(cache_video, video)
    rim = lax.ppermute(rim, HA, up)
    ends = jnp.broadcast_to(
        jnp.stack([place > 0, place < devices - 1]).astype(F32)[:, None], (2, c_out)
    )
    kernel_down, ends = lax.optimization_barrier((kernel_down, ends))
    kernel_down = pltpu.with_memory_space_constraint(kernel_down, pltpu.HBM)
    line = whole((frames, half, c_out), F32)
    edge = whole((cached + 2 * frames, half, c_out), BF16)
    message = whole((1, LANES), F32)
    row, part, third, center, sums, below = pl.pallas_call(
        down_kernel,
        name="down",
        out_shape=(
            line,
            line,
            whole((3, 3, c_in, c_out), BF16),
            whole((1, c_out), F32),
            whole((2, c_out), F32),
            edge,
        ),
        in_specs=[HBM] * 4,
        out_specs=(AUTO,) * 6,
        scratch_shapes=[
            pltpu.VMEM(cache_video.shape, BF16),
            pltpu.VMEM(video.shape, BF16),
            pltpu.VMEM((3, 2, 3, c_in, c_out), BF16),
            pltpu.VMEM((cached + frames, rows, half, 2 * c_in), BF16),
            DMA((5,)),
        ],
        compiler_params=limit(24),
        cost_estimate=pl.CostEstimate(flops=2 * 10**9, bytes_accessed=4 * 10**6, transcendentals=0),
    )(cache_video, video, kernel_down, cache_hidden)
    below = lax.ppermute(below, HA, up)
    last, above, stats = pl.pallas_call(
        rim_down_kernel,
        name="rim_down",
        out_shape=(line, edge, message),
        in_specs=[AUTO] * 5 + [HBM],
        out_specs=(AUTO,) * 3,
        scratch_shapes=[pltpu.VMEM((cached + frames, half, 2 * c_in), BF16), DMA(())],
        compiler_params=limit(16),
    )(rim, third, part, center, sums, cache_hidden)
    above = lax.ppermute(above, HA, down)
    stats = everyone(stats)
    second, next_cache, stats = pl.pallas_call(
        mix_kernel,
        name="mix",
        out_shape=(whole((frames, 2, half, c_out), F32), whole((2, 2, half, c_out), BF16), message),
        in_specs=[AUTO] * 8 + [HBM] * 2,
        out_specs=(AUTO, ANY, AUTO),
        scratch_shapes=[
            pltpu.VMEM((cached + frames, 4, half, c_out), BF16),
            pltpu.VMEM((3, 3, 3, c_out, c_out), BF16),
            DMA((5,)),
        ],
        compiler_params=limit(28),
    )(row, last, above, below, ends, stats, gain_down[None], shift_down[None], cache_hidden, kernel_mix)
    stats = everyone(stats)
    encoded = pl.pallas_call(
        final_kernel,
        name="final",
        out_shape=whole((frames, 2, half, c_out), BF16),
        in_specs=[AUTO] * 4,
        out_specs=ANY,
        scratch_shapes=[pltpu.VMEM((frames, 2, half, c_out), BF16), DMA((frames,))],
        compiler_params=limit(8),
    )(second, stats, gain_mix[None], shift_mix[None])
    return (encoded, next_cache)


def solution(mesh):
    split = Mesh(
        mesh.devices.reshape(mesh.shape["groups"], 8, 8, 2), ("groups", "ha_0", "ha_1", "ha_2")
    )
    strips = P("groups", HA, None, None)

    return jax.shard_map(
        local,
        mesh=split,
        in_specs=(strips, strips, strips, P(), P(), P(), P(), P(), P()),
        out_specs=(strips, strips),
        check_vma=False,
    )
```

```python
import jax
import jax.numpy as jnp
from jax import lax
from jax.experimental import pallas as pl
from jax.experimental.pallas import tpu as pltpu
from jax.sharding import Mesh
from jax.sharding import PartitionSpec as P

GROUPS = 32
LANES = 128
EPS = 1e-6
HA = ("ha_0", "ha_1", "ha_2")
F32 = jnp.float32
BF16 = jnp.bfloat16
AUTO = pl.BlockSpec()
ANY = pl.BlockSpec(memory_space=pl.ANY)
HBM = pl.BlockSpec(memory_space=pltpu.HBM)
DMA = pltpu.SemaphoreType.DMA


def limit(mib):
    return pltpu.CompilerParams(vmem_limit_bytes=mib * 2**20)


def lanes_of(x):
    return lax.broadcasted_iota(jnp.int32, x.shape, x.ndim - 1)


def turn(x, by):
    return pltpu.roll(x, by % x.shape[-1], x.ndim - 1)


def group_sum(x):
    lane = lanes_of(x)
    step = 1
    while step < x.shape[-1] // GROUPS:
        x = x + jnp.where((lane & step) != 0, turn(x, step), turn(x, -step))
        step *= 2
    return x


def column_sum(block):
    return jnp.sum(block, axis=0, keepdims=True)


def moments_row(center, sums, squares, count):
    members = count * (center.shape[-1] // GROUPS)
    shift = group_sum(sums) * (1.0 / members)
    squares = group_sum(squares) - shift * shift * members
    mean = center + shift
    kind = lanes_of(mean[:, :LANES]) % 4
    low = jnp.where(kind == 0, mean[:, :LANES], squares[:, :LANES])
    high = jnp.where(kind == 2, mean[:, LANES:], squares[:, LANES:])
    return jnp.where(kind < 2, low, high)


def affine(rows, members, gain):
    devices = rows.shape[0]
    total = column_sum(rows)
    center = total * (1.0 / devices)
    off = rows - center
    between = column_sum(off * off) * members
    spread = (total + turn(between, 1)) * (1.0 / (members * devices))
    rate = lax.rsqrt(jnp.maximum(spread, 0.0) + EPS)
    kind = lanes_of(total) % 4

    def fill(value, at):
        value = jnp.where(kind == at, value, 0.0)
        value = value + turn(value, 1 if at % 2 == 0 else -1)
        return value + turn(value, 2 if at < 2 else -2)

    centers = jnp.concatenate([fill(center, 0), fill(center, 2)], axis=1)
    rates = jnp.concatenate([fill(rate, 1), fill(rate, 3)], axis=1)
    return centers, rates * gain


def silu_norm(values, center, factor, offset):
    normed = (values - center) * factor + offset
    return normed / (1.0 + jnp.exp(-normed))


def shift_back(x):
    rows = x.shape[0]
    place = lax.broadcasted_iota(jnp.int32, x.shape, 0)
    return jnp.where(place == rows - 1, 0.0, pltpu.roll(x, rows - 1, 0))


def shift_on(x):
    place = lax.broadcasted_iota(jnp.int32, x.shape, 0)
    return jnp.where(place == 0, 0.0, pltpu.roll(x, 1, 0))


def rim_kernel(cache_ref, video_ref, out_ref, sems):
    cached = cache_ref.shape[0]
    copies = [
        pltpu.make_async_copy(cache_ref.at[:, 0], out_ref.at[:cached], sems.at[0]),
        pltpu.make_async_copy(video_ref.at[:, 0], out_ref.at[cached:], sems.at[1]),
    ]
    for c in copies:
        c.start()
    for c in copies:
        c.wait()


def pair_up(source, target, c_in):
    half = target.shape[0]
    target[:, :c_in] = source[pl.ds(0, half, stride=2), :]
    target[:, c_in:] = source[pl.ds(1, half, stride=2), :]


def split_in_two(value):
    coarse = value.astype(BF16)
    return coarse, (value - coarse.astype(F32)).astype(BF16)


def down_kernel(
    cache_ref, video_ref, kernel_ref, hidden_ref,
    row_ref, part_ref, third_ref, center_ref, sums_ref, edge_ref,
    cache_buf, video_buf, kernel_buf, pairs_ref, sems,
):
    frames, rows, width, c_in = video_ref.shape
    cached = cache_ref.shape[0]
    half = width // 2
    c_out = kernel_ref.shape[-1]
    loads = [
        pltpu.make_async_copy(cache_ref, cache_buf, sems.at[0]),
        pltpu.make_async_copy(video_ref, video_buf, sems.at[1]),
        pltpu.make_async_copy(kernel_ref.at[:, :2], kernel_buf, sems.at[2]),
        pltpu.make_async_copy(kernel_ref.at[:, 2], third_ref, sems.at[3]),
        pltpu.make_async_copy(hidden_ref.at[:, 0], edge_ref.at[:cached], sems.at[4]),
    ]
    for c in loads:
        c.start()
    for f in range(cached + frames):
        if f == 0:
            loads[0].wait()
        if f == cached:
            loads[1].wait()
        for r in range(rows):
            source = cache_buf.at[f, r] if f < cached else video_buf.at[f - cached, r]
            pair_up(source, pairs_ref.at[f, r], c_in)
    loads[2].wait()
    loads[3].wait()

    def tap(a, b, c):
        return third_ref[a, c] if b == 2 else kernel_buf[a, b, c]

    for i, depth in ((0, 3), (1, 2)):
        where = [(a, b) for b in range(depth) for a in range(3)]
        taps = [pairs_ref[a : a + frames, 2 * i + b].reshape(frames * half, 2 * c_in) for a, b in where]
        both = jnp.concatenate([tap(a, b, c) for a, b in where for c in range(2)], axis=0)
        ahead = jnp.concatenate([tap(a, b, 2) for a, b in where], axis=0)
        here = jnp.dot(jnp.concatenate(taps, axis=1), both, preferred_element_type=F32)
        evens = jnp.concatenate([t[:, :c_in] for t in taps], axis=1)
        after = jnp.dot(evens, ahead, preferred_element_type=F32)
        for t in range(frames):
            span = slice(t * half, (t + 1) * half)
            block = here[span] + shift_back(after[span])
            if i == 0:
                row_ref[t] = block
                edge_ref[cached + t], edge_ref[cached + frames + t] = split_in_two(block)
            else:
                part_ref[t] = block
    total = sum(column_sum(row_ref[t]) for t in range(frames))
    center = group_sum(total) * (1.0 / (frames * half * (c_out // GROUPS)))
    center_ref[...] = center
    sums_ref[0:1] = total - center * (frames * half)
    sums_ref[1:2] = sum(column_sum((row_ref[t] - center) ** 2) for t in range(frames))
    loads[4].wait()


def rim_down_kernel(
    rim_ref, ends_ref, third_ref, part_ref, center_ref, sums_ref, hidden_ref,
    last_ref, edge_ref, message_ref,
    pairs_ref, sem,
):
    frames, half, _ = part_ref.shape
    c_in = rim_ref.shape[-1]
    cached, rows = hidden_ref.shape[:2]
    load = pltpu.make_async_copy(hidden_ref.at[:, rows - 1], edge_ref.at[:cached], sem)
    load.start()
    for f in range(rim_ref.shape[0]):
        pair_up(rim_ref.at[f], pairs_ref.at[f], c_in)
    taps = [pairs_ref[a : a + frames].reshape(frames * half, 2 * c_in) for a in range(3)]
    both = jnp.concatenate([third_ref[a, c] for a in range(3) for c in range(2)], axis=0)
    ahead = jnp.concatenate([third_ref[a, 2] for a in range(3)], axis=0)
    here = jnp.dot(jnp.concatenate(taps, axis=1), both, preferred_element_type=F32)
    evens = jnp.concatenate([t[:, :c_in] for t in taps], axis=1)
    after = jnp.dot(evens, ahead, preferred_element_type=F32)
    keep = ends_ref[1:2]
    center = center_ref[...]
    sums, squares = sums_ref[0:1], sums_ref[1:2]
    for t in range(frames):
        span = slice(t * half, (t + 1) * half)
        block = part_ref[t] + jnp.where(keep > 0, here[span] + shift_back(after[span]), 0.0)
        last_ref[t] = block
        edge_ref[cached + t], edge_ref[cached + frames + t] = split_in_two(block)
        off = block - center
        sums = sums + column_sum(off)
        squares = squares + column_sum(off * off)
    message_ref[...] = moments_row(center, sums, squares, 2 * frames * half)
    load.wait()


def unpack(stats_ref):
    both = stats_ref[...][:, 0]
    return jnp.concatenate([both[:, :LANES], both[:, LANES:]], axis=0)


def mix_kernel(
    row_ref, last_ref, above_ref, below_ref, ends_ref, stats_ref, gain_ref, shift_ref, hidden_ref, kernel_ref,
    second_ref, next_ref, message_ref,
    rows_ref, sems,
):
    frames, width, channels = row_ref.shape
    cached = hidden_ref.shape[0]
    rows = 2
    count = rows * frames * width
    load = pltpu.make_async_copy(hidden_ref, rows_ref.at[:cached, 1 : 1 + rows], sems.at[0])
    load.start()
    keep_above, keep_below = ends_ref[0:1], ends_ref[1:2]
    for f in range(cached):
        rows_ref[f, 0] = jnp.where(keep_above > 0, above_ref[f].astype(F32), 0.0).astype(BF16)
        rows_ref[f, rows + 1] = jnp.where(keep_below > 0, below_ref[f].astype(F32), 0.0).astype(BF16)
    center, factor = affine(unpack(stats_ref), count * (channels // GROUPS), gain_ref[...])
    offset = shift_ref[...]

    def activate(t):
        for at, edge_ref, keep in ((0, above_ref, keep_above), (rows + 1, below_ref, keep_below)):
            value = edge_ref[cached + t].astype(F32) + edge_ref[cached + frames + t].astype(F32)
            hidden = silu_norm(value, center, factor, offset)
            rows_ref[cached + t, at] = jnp.where(keep > 0, hidden, 0.0).astype(BF16)
        rows_ref[cached + t, 1] = silu_norm(row_ref[t], center, factor, offset).astype(BF16)
        rows_ref[cached + t, 2] = silu_norm(last_ref[t], center, factor, offset).astype(BF16)

    step = frames // 2
    for begin in range(0, frames, step):
        for t in range(begin, begin + step):
            activate(t)
        if begin == 0:
            load.wait()
        taps = jnp.concatenate(
            [
                rows_ref[begin + a : begin + a + step, b : b + rows].reshape(step * rows * width, channels)
                for a in range(3)
                for b in range(3)
            ],
            axis=1,
        )
        parts = []
        for c in range(3):
            weights = jnp.concatenate([kernel_ref[a, b, c] for a in range(3) for b in range(3)], axis=0)
            parts.append(jnp.dot(taps, weights, preferred_element_type=F32))
        left, here, right = parts
        for n in range(step * rows):
            span = slice(n * width, (n + 1) * width)
            t, i = begin + n // rows, n % rows
            second_ref[t, i] = here[span] + shift_on(left[span]) + shift_back(right[span])
        if begin == 0:
            blocks = [second_ref[t, i] for t in range(step) for i in range(rows)]
            total = sum(column_sum(b) for b in blocks)
            middle = group_sum(total) * (2.0 / (count * (channels // GROUPS)))
    store = pltpu.make_async_copy(
        rows_ref.at[cached + frames - 2 : cached + frames, 1 : 1 + rows], next_ref, sems.at[1]
    )
    store.start()
    offs = [second_ref[t, i] - middle for t in range(frames) for i in range(rows)]
    sums = sum(column_sum(off) for off in offs)
    squares = sum(column_sum(off * off) for off in offs)
    message_ref[...] = moments_row(middle, sums, squares, count)
    store.wait()


def final_kernel(second_ref, stats_ref, gain_ref, shift_ref, out_ref, buf, sems):
    frames, rows, width, channels = second_ref.shape
    members = frames * rows * width * (channels // GROUPS)
    center, factor = affine(unpack(stats_ref), members, gain_ref[...])
    offset = shift_ref[...]
    stores = []
    for t in range(frames):
        for i in range(rows):
            buf[t, i] = silu_norm(second_ref[t, i], center, factor, offset).astype(BF16)
        stores.append(pltpu.make_async_copy(buf.at[t], out_ref.at[t], sems.at[t]))
        stores[-1].start()
    for c in stores:
        c.wait()


def both_kernel(mine_ref, other_ref, out_ref):
    both = jnp.concatenate([mine_ref[...], other_ref[...]], axis=1)
    out_ref[...] = jnp.broadcast_to(both[None], out_ref.shape)


def everyone(message):
    devices, chips = lax.axis_size(HA), lax.axis_size(HA[:-1])
    other = lax.ppermute(message, HA, [(i, i ^ 1) for i in range(devices)])
    copies = pl.pallas_call(
        both_kernel,
        name="both",
        out_shape=jax.ShapeDtypeStruct((chips, 1, 2 * LANES), F32),
        in_specs=[AUTO] * 2,
        out_specs=AUTO,
        compiler_params=limit(1),
    )(message, other)
    return lax.all_to_all(copies, HA[:-1], 0, 0)


def local(video, cache_video, cache_hidden, kernel_down, gain_down, shift_down, kernel_mix, gain_mix, shift_mix):
    frames, rows, width, c_in = video.shape
    cached = cache_video.shape[0]
    c_out = kernel_down.shape[-1]
    half = width // 2
    video, cache_video, cache_hidden = (
        pltpu.with_memory_space_constraint(x, pltpu.HBM) for x in (video, cache_video, cache_hidden)
    )
    devices = lax.axis_size(HA)
    place = lax.axis_index(HA)
    up = [((i + 1) % devices, i) for i in range(devices)]
    down = [(i, (i + 1) % devices) for i in range(devices)]
    whole = jax.ShapeDtypeStruct
    rim = pl.pallas_call(
        rim_kernel,
        name="rim",
        out_shape=whole((cached + frames, width, c_in), BF16),
        in_specs=[HBM] * 2,
        out_specs=AUTO,
        scratch_shapes=[DMA((2,))],
        compiler_params=limit(4),
    )(cache_video, video)
    rim = lax.ppermute(rim, HA, up)
    ends = jnp.broadcast_to(
        jnp.stack([place > 0, place < devices - 1]).astype(F32)[:, None], (2, c_out)
    )
    kernel_down, ends = lax.optimization_barrier((kernel_down, ends))
    kernel_down = pltpu.with_memory_space_constraint(kernel_down, pltpu.HBM)
    line = whole((frames, half, c_out), F32)
    edge = whole((cached + 2 * frames, half, c_out), BF16)
    message = whole((1, LANES), F32)
    row, part, third, center, sums, below = pl.pallas_call(
        down_kernel,
        name="down",
        out_shape=(
            line,
            line,
            whole((3, 3, c_in, c_out), BF16),
            whole((1, c_out), F32),
            whole((2, c_out), F32),
            edge,
        ),
        in_specs=[HBM] * 4,
        out_specs=(AUTO,) * 6,
        scratch_shapes=[
            pltpu.VMEM(cache_video.shape, BF16),
            pltpu.VMEM(video.shape, BF16),
            pltpu.VMEM((3, 2, 3, c_in, c_out), BF16),
            pltpu.VMEM((cached + frames, rows, half, 2 * c_in), BF16),
            DMA((5,)),
        ],
        compiler_params=limit(24),
        cost_estimate=pl.CostEstimate(flops=2 * 10**9, bytes_accessed=4 * 10**6, transcendentals=0),
    )(cache_video, video, kernel_down, cache_hidden)
    below = lax.ppermute(below, HA, up)
    last, above, stats = pl.pallas_call(
        rim_down_kernel,
        name="rim_down",
        out_shape=(line, edge, message),
        in_specs=[AUTO] * 6 + [HBM],
        out_specs=(AUTO,) * 3,
        scratch_shapes=[pltpu.VMEM((cached + frames, half, 2 * c_in), BF16), DMA(())],
        compiler_params=limit(16),
    )(rim, ends, third, part, center, sums, cache_hidden)
    above = lax.ppermute(above, HA, down)
    stats = everyone(stats)
    second, next_cache, stats = pl.pallas_call(
        mix_kernel,
        name="mix",
        out_shape=(whole((frames, 2, half, c_out), F32), whole((2, 2, half, c_out), BF16), message),
        in_specs=[AUTO] * 8 + [HBM, AUTO],
        out_specs=(AUTO, ANY, AUTO),
        scratch_shapes=[
            pltpu.VMEM((cached + frames, 4, half, c_out), BF16),
            DMA((2,)),
        ],
        compiler_params=limit(28),
    )(row, last, above, below, ends, stats, gain_down[None], shift_down[None], cache_hidden, kernel_mix)
    stats = everyone(stats)
    encoded = pl.pallas_call(
        final_kernel,
        name="final",
        out_shape=whole((frames, 2, half, c_out), BF16),
        in_specs=[AUTO] * 4,
        out_specs=ANY,
        scratch_shapes=[pltpu.VMEM((frames, 2, half, c_out), BF16), DMA((frames,))],
        compiler_params=limit(8),
    )(second, stats, gain_mix[None], shift_mix[None])
    return (encoded, next_cache)


def solution(mesh):
    split = Mesh(
        mesh.devices.reshape(mesh.shape["groups"], 8, 8, 2), ("groups", "ha_0", "ha_1", "ha_2")
    )
    strips = P("groups", HA, None, None)

    return jax.shard_map(
        local,
        mesh=split,
        in_specs=(strips, strips, strips, P(), P(), P(), P(), P(), P()),
        out_specs=(strips, strips),
        check_vma=False,
    )
```

```python
import jax
import jax.numpy as jnp
from jax import lax
from jax.experimental import pallas as pl
from jax.experimental.pallas import tpu as pltpu
from jax.sharding import Mesh
from jax.sharding import PartitionSpec as P

GROUPS = 32
LANES = 128
EPS = 1e-6
HA = ("ha_0", "ha_1", "ha_2")
F32 = jnp.float32
BF16 = jnp.bfloat16
AUTO = pl.BlockSpec()
ANY = pl.BlockSpec(memory_space=pl.ANY)
HBM = pl.BlockSpec(memory_space=pltpu.HBM)
DMA = pltpu.SemaphoreType.DMA


def limit(mib):
    return pltpu.CompilerParams(vmem_limit_bytes=mib * 2**20)


def lanes_of(x):
    return lax.broadcasted_iota(jnp.int32, x.shape, x.ndim - 1)


def turn(x, by):
    return pltpu.roll(x, by % x.shape[-1], x.ndim - 1)


def group_sum(x):
    lane = lanes_of(x)
    step = 1
    while step < x.shape[-1] // GROUPS:
        x = x + jnp.where((lane & step) != 0, turn(x, step), turn(x, -step))
        step *= 2
    return x


def column_sum(block):
    return jnp.sum(block, axis=0, keepdims=True)


def moments_row(center, sums, squares, count):
    members = count * (center.shape[-1] // GROUPS)
    shift = group_sum(sums) * (1.0 / members)
    squares = group_sum(squares) - shift * shift * members
    mean = center + shift
    kind = lanes_of(mean[:, :LANES]) % 4
    low = jnp.where(kind == 0, mean[:, :LANES], squares[:, :LANES])
    high = jnp.where(kind == 2, mean[:, LANES:], squares[:, LANES:])
    return jnp.where(kind < 2, low, high)


def affine(rows, members, gain):
    devices = rows.shape[0]
    total = column_sum(rows)
    center = total * (1.0 / devices)
    off = rows - center
    between = column_sum(off * off) * members
    spread = (total + turn(between, 1)) * (1.0 / (members * devices))
    rate = lax.rsqrt(jnp.maximum(spread, 0.0) + EPS)
    kind = lanes_of(total) % 4

    def fill(value, at):
        value = jnp.where(kind == at, value, 0.0)
        value = value + turn(value, 1 if at % 2 == 0 else -1)
        return value + turn(value, 2 if at < 2 else -2)

    centers = jnp.concatenate([fill(center, 0), fill(center, 2)], axis=1)
    rates = jnp.concatenate([fill(rate, 1), fill(rate, 3)], axis=1)
    return centers, rates * gain


def silu_norm(values, center, factor, offset):
    normed = (values - center) * factor + offset
    return normed / (1.0 + jnp.exp(-normed))


def shift_back(x):
    rows = x.shape[0]
    place = lax.broadcasted_iota(jnp.int32, x.shape, 0)
    return jnp.where(place == rows - 1, 0.0, pltpu.roll(x, rows - 1, 0))


def shift_on(x):
    place = lax.broadcasted_iota(jnp.int32, x.shape, 0)
    return jnp.where(place == 0, 0.0, pltpu.roll(x, 1, 0))


def rim_kernel(cache_ref, video_ref, out_ref, sems):
    cached = cache_ref.shape[0]
    copies = [
        pltpu.make_async_copy(cache_ref.at[:, 0], out_ref.at[:cached], sems.at[0]),
        pltpu.make_async_copy(video_ref.at[:, 0], out_ref.at[cached:], sems.at[1]),
    ]
    for c in copies:
        c.start()
    for c in copies:
        c.wait()


def pair_up(source, target, c_in):
    half = target.shape[0]
    target[:, :c_in] = source[pl.ds(0, half, stride=2), :]
    target[:, c_in:] = source[pl.ds(1, half, stride=2), :]


def split_in_two(value):
    coarse = value.astype(BF16)
    return coarse, (value - coarse.astype(F32)).astype(BF16)


def down_kernel(
    cache_ref, video_ref, kernel_ref, hidden_ref,
    row_ref, part_ref, third_ref, center_ref, sums_ref, edge_ref,
    cache_buf, video_buf, kernel_buf, pairs_ref, sems,
):
    frames, rows, width, c_in = video_ref.shape
    cached = cache_ref.shape[0]
    half = width // 2
    c_out = kernel_ref.shape[-1]
    loads = [
        pltpu.make_async_copy(cache_ref, cache_buf, sems.at[0]),
        pltpu.make_async_copy(video_ref, video_buf, sems.at[1]),
        pltpu.make_async_copy(kernel_ref.at[:, :2], kernel_buf, sems.at[2]),
        pltpu.make_async_copy(kernel_ref.at[:, 2], third_ref, sems.at[3]),
        pltpu.make_async_copy(hidden_ref.at[:, 0], edge_ref.at[:cached], sems.at[4]),
    ]
    for c in loads:
        c.start()
    for f in range(cached + frames):
        if f == 0:
            loads[0].wait()
        if f == cached:
            loads[1].wait()
        for r in range(rows):
            source = cache_buf.at[f, r] if f < cached else video_buf.at[f - cached, r]
            pair_up(source, pairs_ref.at[f, r], c_in)
    loads[2].wait()
    loads[3].wait()

    def tap(a, b, c):
        return third_ref[a, c] if b == 2 else kernel_buf[a, b, c]

    for i, depth in ((0, 3), (1, 2)):
        where = [(a, b) for b in range(depth) for a in range(3)]
        taps = [pairs_ref[a : a + frames, 2 * i + b].reshape(frames * half, 2 * c_in) for a, b in where]
        both = jnp.concatenate([tap(a, b, c) for a, b in where for c in range(2)], axis=0)
        ahead = jnp.concatenate([tap(a, b, 2) for a, b in where], axis=0)
        here = jnp.dot(jnp.concatenate(taps, axis=1), both, preferred_element_type=F32)
        evens = jnp.concatenate([t[:, :c_in] for t in taps], axis=1)
        after = jnp.dot(evens, ahead, preferred_element_type=F32)
        for t in range(frames):
            span = slice(t * half, (t + 1) * half)
            block = here[span] + shift_back(after[span])
            if i == 0:
                row_ref[t] = block
                edge_ref[cached + t], edge_ref[cached + frames + t] = split_in_two(block)
            else:
                part_ref[t] = block
    total = sum(column_sum(row_ref[t]) for t in range(frames))
    center = group_sum(total) * (1.0 / (frames * half * (c_out // GROUPS)))
    center_ref[...] = center
    sums_ref[0:1] = total - center * (frames * half)
    sums_ref[1:2] = sum(column_sum((row_ref[t] - center) ** 2) for t in range(frames))
    loads[4].wait()


def rim_down_kernel(
    rim_ref, ends_ref, third_ref, part_ref, center_ref, sums_ref, hidden_ref,
    last_ref, edge_ref, message_ref,
    pairs_ref,
):
    frames, half, _ = part_ref.shape
    c_in = rim_ref.shape[-1]
    cached, rows = hidden_ref.shape[:2]
    for f in range(cached):
        edge_ref[f] = hidden_ref[f, rows - 1]
    for f in range(rim_ref.shape[0]):
        pair_up(rim_ref.at[f], pairs_ref.at[f], c_in)
    taps = [pairs_ref[a : a + frames].reshape(frames * half, 2 * c_in) for a in range(3)]
    both = jnp.concatenate([third_ref[a, c] for a in range(3) for c in range(2)], axis=0)
    ahead = jnp.concatenate([third_ref[a, 2] for a in range(3)], axis=0)
    here = jnp.dot(jnp.concatenate(taps, axis=1), both, preferred_element_type=F32)
    evens = jnp.concatenate([t[:, :c_in] for t in taps], axis=1)
    after = jnp.dot(evens, ahead, preferred_element_type=F32)
    keep = ends_ref[1:2]
    center = center_ref[...]
    sums, squares = sums_ref[0:1], sums_ref[1:2]
    for t in range(frames):
        span = slice(t * half, (t + 1) * half)
        block = part_ref[t] + jnp.where(keep > 0, here[span] + shift_back(after[span]), 0.0)
        last_ref[t] = block
        edge_ref[cached + t], edge_ref[cached + frames + t] = split_in_two(block)
        off = block - center
        sums = sums + column_sum(off)
        squares = squares + column_sum(off * off)
    message_ref[...] = moments_row(center, sums, squares, 2 * frames * half)


def unpack(stats_ref):
    both = stats_ref[...][:, 0]
    return jnp.concatenate([both[:, :LANES], both[:, LANES:]], axis=0)


def mix_kernel(
    row_ref, last_ref, above_ref, below_ref, ends_ref, stats_ref, gain_ref, shift_ref, hidden_ref, kernel_ref,
    second_ref, next_ref, message_ref,
    rows_ref, sem,
):
    frames, width, channels = row_ref.shape
    cached = hidden_ref.shape[0]
    rows = 2
    count = rows * frames * width
    for f in range(cached):
        for i in range(rows):
            rows_ref[f, 1 + i] = hidden_ref[f, i]
    keep_above, keep_below = ends_ref[0:1], ends_ref[1:2]
    for f in range(cached):
        rows_ref[f, 0] = above_ref[f] * keep_above.astype(BF16)
        rows_ref[f, rows + 1] = below_ref[f] * keep_below.astype(BF16)
    center, factor = affine(unpack(stats_ref), count * (channels // GROUPS), gain_ref[...])
    offset = shift_ref[...]

    def activate(t):
        for at, edge_ref, keep in ((0, above_ref, keep_above), (rows + 1, below_ref, keep_below)):
            value = edge_ref[cached + t].astype(F32) + edge_ref[cached + frames + t].astype(F32)
            hidden = silu_norm(value, center, factor, offset)
            rows_ref[cached + t, at] = jnp.where(keep > 0, hidden, 0.0).astype(BF16)
        rows_ref[cached + t, 1] = silu_norm(row_ref[t], center, factor, offset).astype(BF16)
        rows_ref[cached + t, 2] = silu_norm(last_ref[t], center, factor, offset).astype(BF16)

    step = frames // 2
    for begin in range(0, frames, step):
        for t in range(begin, begin + step):
            activate(t)
        taps = jnp.concatenate(
            [
                rows_ref[begin + a : begin + a + step, b : b + rows].reshape(step * rows * width, channels)
                for a in range(3)
                for b in range(3)
            ],
            axis=1,
        )
        parts = []
        for c in range(3):
            weights = jnp.concatenate([kernel_ref[a, b, c] for a in range(3) for b in range(3)], axis=0)
            parts.append(jnp.dot(taps, weights, preferred_element_type=F32))
        left, here, right = parts
        for n in range(step * rows):
            span = slice(n * width, (n + 1) * width)
            t, i = begin + n // rows, n % rows
            second_ref[t, i] = here[span] + shift_on(left[span]) + shift_back(right[span])
        if begin == 0:
            blocks = [second_ref[t, i] for t in range(step) for i in range(rows)]
            total = sum(column_sum(b) for b in blocks)
            middle = group_sum(total) * (2.0 / (count * (channels // GROUPS)))
    store = pltpu.make_async_copy(
        rows_ref.at[cached + frames - 2 : cached + frames, 1 : 1 + rows], next_ref, sem
    )
    store.start()
    offs = [second_ref[t, i] - middle for t in range(frames) for i in range(rows)]
    sums = sum(column_sum(off) for off in offs)
    squares = sum(column_sum(off * off) for off in offs)
    message_ref[...] = moments_row(middle, sums, squares, count)
    store.wait()


def final_kernel(second_ref, stats_ref, gain_ref, shift_ref, out_ref, buf, sems):
    frames, rows, width, channels = second_ref.shape
    members = frames * rows * width * (channels // GROUPS)
    center, factor = affine(unpack(stats_ref), members, gain_ref[...])
    offset = shift_ref[...]
    stores = []
    for t in range(frames):
        for i in range(rows):
            buf[t, i] = silu_norm(second_ref[t, i], center, factor, offset).astype(BF16)
        stores.append(pltpu.make_async_copy(buf.at[t], out_ref.at[t], sems.at[t]))
        stores[-1].start()
    for c in stores:
        c.wait()


def both_kernel(mine_ref, other_ref, out_ref):
    both = jnp.concatenate([mine_ref[...], other_ref[...]], axis=1)
    out_ref[...] = jnp.broadcast_to(both[None], out_ref.shape)


def everyone(message):
    devices, chips = lax.axis_size(HA), lax.axis_size(HA[:-1])
    other = lax.ppermute(message, HA, [(i, i ^ 1) for i in range(devices)])
    copies = pl.pallas_call(
        both_kernel,
        name="both",
        out_shape=jax.ShapeDtypeStruct((chips, 1, 2 * LANES), F32),
        in_specs=[AUTO] * 2,
        out_specs=AUTO,
        compiler_params=limit(1),
    )(message, other)
    return lax.all_to_all(copies, HA[:-1], 0, 0)


def run_mix(row, last, above, below, ends, stats, gain, shift, hidden, kernel):
    frames, half, c_out = row.shape
    cached = hidden.shape[0]
    whole = jax.ShapeDtypeStruct
    return pl.pallas_call(
        mix_kernel,
        name="mix",
        out_shape=(
            whole((frames, 2, half, c_out), F32),
            whole((2, 2, half, c_out), BF16),
            whole((1, LANES), F32),
        ),
        in_specs=[AUTO] * 10,
        out_specs=(AUTO, ANY, AUTO),
        scratch_shapes=[pltpu.VMEM((cached + frames, 4, half, c_out), BF16), DMA(())],
        compiler_params=limit(28),
    )(row, last, above, below, ends, stats, gain, shift, hidden, kernel)


def local(video, cache_video, cache_hidden, kernel_down, gain_down, shift_down, kernel_mix, gain_mix, shift_mix):
    frames, rows, width, c_in = video.shape
    cached = cache_video.shape[0]
    c_out = kernel_down.shape[-1]
    half = width // 2
    video, cache_video, stored_hidden = (
        pltpu.with_memory_space_constraint(x, pltpu.HBM) for x in (video, cache_video, cache_hidden)
    )
    devices = lax.axis_size(HA)
    place = lax.axis_index(HA)
    up = [((i + 1) % devices, i) for i in range(devices)]
    down = [(i, (i + 1) % devices) for i in range(devices)]
    whole = jax.ShapeDtypeStruct
    rim = pl.pallas_call(
        rim_kernel,
        name="rim",
        out_shape=whole((cached + frames, width, c_in), BF16),
        in_specs=[HBM] * 2,
        out_specs=AUTO,
        scratch_shapes=[DMA((2,))],
        compiler_params=limit(4),
    )(cache_video, video)
    rim = lax.ppermute(rim, HA, up)
    ends = jnp.broadcast_to(
        jnp.stack([place > 0, place < devices - 1]).astype(F32)[:, None], (2, c_out)
    )
    kernel_down, ends = lax.optimization_barrier((kernel_down, ends))
    kernel_down = pltpu.with_memory_space_constraint(kernel_down, pltpu.HBM)
    line = whole((frames, half, c_out), F32)
    edge = whole((cached + 2 * frames, half, c_out), BF16)
    message = whole((1, LANES), F32)
    row, part, third, center, sums, below = pl.pallas_call(
        down_kernel,
        name="down",
        out_shape=(
            line,
            line,
            whole((3, 3, c_in, c_out), BF16),
            whole((1, c_out), F32),
            whole((2, c_out), F32),
            edge,
        ),
        in_specs=[HBM] * 4,
        out_specs=(AUTO,) * 6,
        scratch_shapes=[
            pltpu.VMEM(cache_video.shape, BF16),
            pltpu.VMEM(video.shape, BF16),
            pltpu.VMEM((3, 2, 3, c_in, c_out), BF16),
            pltpu.VMEM((cached + frames, rows, half, 2 * c_in), BF16),
            DMA((5,)),
        ],
        compiler_params=limit(24),
        cost_estimate=pl.CostEstimate(flops=2 * 10**9, bytes_accessed=4 * 10**6, transcendentals=0),
    )(cache_video, video, kernel_down, stored_hidden)
    below = lax.ppermute(below, HA, up)
    last, above, stats = pl.pallas_call(
        rim_down_kernel,
        name="rim_down",
        out_shape=(line, edge, message),
        in_specs=[AUTO] * 7,
        out_specs=(AUTO,) * 3,
        scratch_shapes=[pltpu.VMEM((cached + frames, half, 2 * c_in), BF16)],
        compiler_params=limit(16),
    )(rim, ends, third, part, center, sums, cache_hidden)
    above = lax.ppermute(above, HA, down)
    stats = everyone(stats)
    second, next_cache, stats = run_mix(
        row, last, above, below, ends, stats, gain_down[None], shift_down[None], cache_hidden, kernel_mix
    )
    stats = everyone(stats)
    encoded = pl.pallas_call(
        final_kernel,
        name="final",
        out_shape=whole((frames, 2, half, c_out), BF16),
        in_specs=[AUTO] * 4,
        out_specs=ANY,
        scratch_shapes=[pltpu.VMEM((frames, 2, half, c_out), BF16), DMA((frames,))],
        compiler_params=limit(8),
    )(second, stats, gain_mix[None], shift_mix[None])
    return (encoded, next_cache)


def solution(mesh):
    split = Mesh(
        mesh.devices.reshape(mesh.shape["groups"], 8, 8, 2), ("groups", "ha_0", "ha_1", "ha_2")
    )
    strips = P("groups", HA, None, None)

    return jax.shard_map(
        local,
        mesh=split,
        in_specs=(strips, strips, strips, P(), P(), P(), P(), P(), P()),
        out_specs=(strips, strips),
        check_vma=False,
    )
```

```python
import jax
import jax.numpy as jnp
from jax import lax
from jax.experimental import pallas as pl
from jax.experimental.pallas import tpu as pltpu
from jax.sharding import Mesh
from jax.sharding import PartitionSpec as P

GROUPS = 32
LANES = 128
EPS = 1e-6
HA = ("ha_0", "ha_1", "ha_2")
F32 = jnp.float32
BF16 = jnp.bfloat16
AUTO = pl.BlockSpec()
ANY = pl.BlockSpec(memory_space=pl.ANY)
HBM = pl.BlockSpec(memory_space=pltpu.HBM)
DMA = pltpu.SemaphoreType.DMA


def limit(mib):
    return pltpu.CompilerParams(vmem_limit_bytes=mib * 2**20)


def lanes_of(x):
    return lax.broadcasted_iota(jnp.int32, x.shape, x.ndim - 1)


def turn(x, by):
    return pltpu.roll(x, by % x.shape[-1], x.ndim - 1)


def group_sum(x):
    lane = lanes_of(x)
    step = 1
    while step < x.shape[-1] // GROUPS:
        x = x + jnp.where((lane & step) != 0, turn(x, step), turn(x, -step))
        step *= 2
    return x


def column_sum(block):
    return jnp.sum(block, axis=0, keepdims=True)


def moments_row(center, sums, squares, count):
    members = count * (center.shape[-1] // GROUPS)
    shift = group_sum(sums) * (1.0 / members)
    squares = group_sum(squares) - shift * shift * members
    mean = center + shift
    kind = lanes_of(mean[:, :LANES]) % 4
    low = jnp.where(kind == 0, mean[:, :LANES], squares[:, :LANES])
    high = jnp.where(kind == 2, mean[:, LANES:], squares[:, LANES:])
    return jnp.where(kind < 2, low, high)


def affine(rows, members, gain):
    devices = rows.shape[0]
    total = column_sum(rows)
    center = total * (1.0 / devices)
    off = rows - center
    between = column_sum(off * off) * members
    spread = (total + turn(between, 1)) * (1.0 / (members * devices))
    rate = lax.rsqrt(jnp.maximum(spread, 0.0) + EPS)
    kind = lanes_of(total) % 4

    def fill(value, at):
        value = jnp.where(kind == at, value, 0.0)
        value = value + turn(value, 1 if at % 2 == 0 else -1)
        return value + turn(value, 2 if at < 2 else -2)

    centers = jnp.concatenate([fill(center, 0), fill(center, 2)], axis=1)
    rates = jnp.concatenate([fill(rate, 1), fill(rate, 3)], axis=1)
    return centers, rates * gain


def silu_norm(values, center, factor, offset):
    normed = (values - center) * factor + offset
    return normed / (1.0 + jnp.exp(-normed))


def shift_back(x):
    rows = x.shape[0]
    place = lax.broadcasted_iota(jnp.int32, x.shape, 0)
    return jnp.where(place == rows - 1, 0.0, pltpu.roll(x, rows - 1, 0))


def shift_on(x):
    place = lax.broadcasted_iota(jnp.int32, x.shape, 0)
    return jnp.where(place == 0, 0.0, pltpu.roll(x, 1, 0))


def rim_kernel(cache_ref, video_ref, out_ref, sems):
    cached = cache_ref.shape[0]
    copies = []
    for f in range(out_ref.shape[0]):
        source = cache_ref.at[f, 0] if f < cached else video_ref.at[f - cached, 0]
        copies.append(pltpu.make_async_copy(source, out_ref.at[f], sems.at[f]))
    for c in copies:
        c.start()
    for c in copies:
        c.wait()


def pair_up(source, target, c_in):
    half = target.shape[0]
    target[:, :c_in] = source[pl.ds(0, half, stride=2), :]
    target[:, c_in:] = source[pl.ds(1, half, stride=2), :]


def split_in_two(value):
    coarse = value.astype(BF16)
    return coarse, (value - coarse.astype(F32)).astype(BF16)


def down_kernel(
    cache_ref, video_ref, kernel_ref, hidden_ref,
    row_ref, part_ref, third_ref, center_ref, sums_ref, edge_ref,
    cache_buf, video_buf, kernel_buf, pairs_ref, sems,
):
    frames, rows, width, c_in = video_ref.shape
    cached = cache_ref.shape[0]
    half = width // 2
    c_out = kernel_ref.shape[-1]
    loads = [
        pltpu.make_async_copy(cache_ref, cache_buf, sems.at[0]),
        pltpu.make_async_copy(video_ref, video_buf, sems.at[1]),
        pltpu.make_async_copy(kernel_ref.at[:, :2], kernel_buf, sems.at[2]),
        pltpu.make_async_copy(kernel_ref.at[:, 2], third_ref, sems.at[3]),
        pltpu.make_async_copy(hidden_ref.at[:, 0], edge_ref.at[:cached], sems.at[4]),
    ]
    for c in loads:
        c.start()
    for f in range(cached + frames):
        if f == 0:
            loads[0].wait()
        if f == cached:
            loads[1].wait()
        for r in range(rows):
            source = cache_buf.at[f, r] if f < cached else video_buf.at[f - cached, r]
            pair_up(source, pairs_ref.at[f, r], c_in)
    loads[2].wait()
    loads[3].wait()

    def tap(a, b, c):
        return third_ref[a, c] if b == 2 else kernel_buf[a, b, c]

    for i, depth in ((0, 3), (1, 2)):
        where = [(a, b) for b in range(depth) for a in range(3)]
        taps = [pairs_ref[a : a + frames, 2 * i + b].reshape(frames * half, 2 * c_in) for a, b in where]
        both = jnp.concatenate([tap(a, b, c) for a, b in where for c in range(2)], axis=0)
        ahead = jnp.concatenate([tap(a, b, 2) for a, b in where], axis=0)
        here = jnp.dot(jnp.concatenate(taps, axis=1), both, preferred_element_type=F32)
        evens = jnp.concatenate([t[:, :c_in] for t in taps], axis=1)
        after = jnp.dot(evens, ahead, preferred_element_type=F32)
        for t in range(frames):
            span = slice(t * half, (t + 1) * half)
            block = here[span] + shift_back(after[span])
            if i == 0:
                row_ref[t] = block
                edge_ref[cached + t], edge_ref[cached + frames + t] = split_in_two(block)
            else:
                part_ref[t] = block
    total = sum(column_sum(row_ref[t]) for t in range(frames))
    center = group_sum(total) * (1.0 / (frames * half * (c_out // GROUPS)))
    center_ref[...] = center
    sums_ref[0:1] = total - center * (frames * half)
    sums_ref[1:2] = sum(column_sum((row_ref[t] - center) ** 2) for t in range(frames))
    loads[4].wait()


def rim_down_kernel(
    near_ref, far_ref, ends_ref, third_ref, part_ref, center_ref, sums_ref, hidden_ref,
    last_ref, edge_ref, message_ref,
    rim_ref, pairs_ref,
):
    frames, half, _ = part_ref.shape
    c_in = near_ref.shape[-1]
    cached, rows = hidden_ref.shape[:2]
    for f in range(cached):
        edge_ref[f] = hidden_ref[f, rows - 1]
    odd = ends_ref[2:3, :c_in].astype(BF16)
    for f in range(rim_ref.shape[0]):
        rim_ref[f] = far_ref[f] * odd + near_ref[f] * (1 - odd)
        pair_up(rim_ref.at[f], pairs_ref.at[f], c_in)
    taps = [pairs_ref[a : a + frames].reshape(frames * half, 2 * c_in) for a in range(3)]
    both = jnp.concatenate([third_ref[a, c] for a in range(3) for c in range(2)], axis=0)
    ahead = jnp.concatenate([third_ref[a, 2] for a in range(3)], axis=0)
    here = jnp.dot(jnp.concatenate(taps, axis=1), both, preferred_element_type=F32)
    evens = jnp.concatenate([t[:, :c_in] for t in taps], axis=1)
    after = jnp.dot(evens, ahead, preferred_element_type=F32)
    keep = ends_ref[1:2]
    center = center_ref[...]
    sums, squares = sums_ref[0:1], sums_ref[1:2]
    for t in range(frames):
        span = slice(t * half, (t + 1) * half)
        block = part_ref[t] + jnp.where(keep > 0, here[span] + shift_back(after[span]), 0.0)
        last_ref[t] = block
        edge_ref[cached + t], edge_ref[cached + frames + t] = split_in_two(block)
        off = block - center
        sums = sums + column_sum(off)
        squares = squares + column_sum(off * off)
    message_ref[...] = moments_row(center, sums, squares, 2 * frames * half)


def unpack(stats_ref):
    both = stats_ref[...][:, 0]
    return jnp.concatenate([both[:, :LANES], both[:, LANES:]], axis=0)


def mix_kernel(
    row_ref, last_ref, above_ref, below_ref, ends_ref, stats_ref, gain_ref, shift_ref, hidden_ref, kernel_ref,
    second_ref, next_ref, message_ref,
    rows_ref, sem,
):
    frames, width, channels = row_ref.shape
    cached = hidden_ref.shape[0]
    rows = 2
    count = rows * frames * width
    for f in range(cached):
        for i in range(rows):
            rows_ref[f, 1 + i] = hidden_ref[f, i]
    keep_above, keep_below = ends_ref[0:1], ends_ref[1:2]
    for f in range(cached):
        rows_ref[f, 0] = above_ref[f] * keep_above.astype(BF16)
        rows_ref[f, rows + 1] = below_ref[f] * keep_below.astype(BF16)
    center, factor = affine(unpack(stats_ref), count * (channels // GROUPS), gain_ref[...])
    offset = shift_ref[...]

    def activate(t):
        for at, edge_ref, keep in ((0, above_ref, keep_above), (rows + 1, below_ref, keep_below)):
            value = edge_ref[cached + t].astype(F32) + edge_ref[cached + frames + t].astype(F32)
            hidden = silu_norm(value, center, factor, offset)
            rows_ref[cached + t, at] = jnp.where(keep > 0, hidden, 0.0).astype(BF16)
        rows_ref[cached + t, 1] = silu_norm(row_ref[t], center, factor, offset).astype(BF16)
        rows_ref[cached + t, 2] = silu_norm(last_ref[t], center, factor, offset).astype(BF16)

    step = frames // 2
    for begin in range(0, frames, step):
        if begin == 0:
            for t in range(step):
                activate(t)
        taps = jnp.concatenate(
            [
                rows_ref[begin + a : begin + a + step, b : b + rows].reshape(step * rows * width, channels)
                for a in range(3)
                for b in range(3)
            ],
            axis=1,
        )
        parts = []
        for c in range(3):
            weights = jnp.concatenate([kernel_ref[a, b, c] for a in range(3) for b in range(3)], axis=0)
            parts.append(jnp.dot(taps, weights, preferred_element_type=F32))
        left, here, right = parts
        if begin == 0:
            for t in range(step, frames):
                activate(t)
        blocks = []
        for n in range(step * rows):
            span = slice(n * width, (n + 1) * width)
            t, i = begin + n // rows, n % rows
            block = here[span] + shift_on(left[span]) + shift_back(right[span])
            second_ref[t, i] = block
            blocks.append(block)
        if begin == 0:
            total = sum(column_sum(b) for b in blocks)
            middle = group_sum(total) * (1.0 / (step * rows * width * (channels // GROUPS)))
            sums = total - middle * (step * rows * width)
            blocks = [second_ref[t, i] for t in range(step) for i in range(rows)]
            squares = sum(column_sum((b - middle) ** 2) for b in blocks)
        else:
            offs = [b - middle for b in blocks]
            sums = sums + sum(column_sum(off) for off in offs)
            squares = squares + sum(column_sum(off * off) for off in offs)
    store = pltpu.make_async_copy(
        rows_ref.at[cached + frames - 2 : cached + frames, 1 : 1 + rows], next_ref, sem
    )
    store.start()
    message_ref[...] = moments_row(middle, sums, squares, count)
    store.wait()


def final_kernel(second_ref, stats_ref, gain_ref, shift_ref, out_ref, buf, sems):
    frames, rows, width, channels = second_ref.shape
    members = frames * rows * width * (channels // GROUPS)
    center, factor = affine(unpack(stats_ref), members, gain_ref[...])
    offset = shift_ref[...]
    stores = []
    for t in range(frames):
        for i in range(rows):
            buf[t, i] = silu_norm(second_ref[t, i], center, factor, offset).astype(BF16)
            stores.append(pltpu.make_async_copy(buf.at[t, i], out_ref.at[t, i], sems.at[t * rows + i]))
            stores[-1].start()
    for c in stores:
        c.wait()


def both_kernel(mine_ref, other_ref, out_ref):
    both = jnp.concatenate([mine_ref[...], other_ref[...]], axis=1)
    out_ref[...] = jnp.broadcast_to(both[None], out_ref.shape)


def everyone(message):
    devices, chips = lax.axis_size(HA), lax.axis_size(HA[:-1])
    other = lax.ppermute(message, HA, [(i, i ^ 1) for i in range(devices)])
    copies = pl.pallas_call(
        both_kernel,
        name="both",
        out_shape=jax.ShapeDtypeStruct((chips, 1, 2 * LANES), F32),
        in_specs=[AUTO] * 2,
        out_specs=AUTO,
        compiler_params=limit(1),
    )(message, other)
    return lax.all_to_all(copies, HA[:-1], 0, 0)


def run_mix(row, last, above, below, ends, stats, gain, shift, hidden, kernel):
    frames, half, c_out = row.shape
    cached = hidden.shape[0]
    whole = jax.ShapeDtypeStruct
    return pl.pallas_call(
        mix_kernel,
        name="mix",
        out_shape=(
            whole((frames, 2, half, c_out), F32),
            whole((2, 2, half, c_out), BF16),
            whole((1, LANES), F32),
        ),
        in_specs=[AUTO] * 10,
        out_specs=(AUTO, ANY, AUTO),
        scratch_shapes=[pltpu.VMEM((cached + frames, 4, half, c_out), BF16), DMA(())],
        compiler_params=limit(28),
    )(row, last, above, below, ends, stats, gain, shift, hidden, kernel)


def local(video, cache_video, cache_hidden, kernel_down, gain_down, shift_down, kernel_mix, gain_mix, shift_mix):
    frames, rows, width, c_in = video.shape
    cached = cache_video.shape[0]
    c_out = kernel_down.shape[-1]
    half = width // 2
    video, cache_video, stored_hidden = (
        pltpu.with_memory_space_constraint(x, pltpu.HBM) for x in (video, cache_video, cache_hidden)
    )
    devices = lax.axis_size(HA)
    place = lax.axis_index(HA)
    up = [((i + 1) % devices, i) for i in range(devices)]
    down = [(i, (i + 1) % devices) for i in range(devices)]
    whole = jax.ShapeDtypeStruct
    rim = pl.pallas_call(
        rim_kernel,
        name="rim",
        out_shape=whole((cached + frames, width, c_in), BF16),
        in_specs=[HBM] * 2,
        out_specs=AUTO,
        scratch_shapes=[DMA((cached + frames,))],
        compiler_params=limit(4),
    )(cache_video, video)
    pairs = [(i, i ^ 1) for i in range(devices)]
    bridges = [(i, min(max(i + (1 if i % 2 else -1), 0), devices - 1)) for i in range(devices)]
    near_rim = lax.ppermute(rim, HA, pairs)
    far_rim = lax.ppermute(rim, HA, bridges)
    ends = jnp.broadcast_to(
        jnp.stack([place > 0, place < devices - 1, place % 2 > 0]).astype(F32)[:, None], (3, c_out)
    )
    kernel_down, ends = lax.optimization_barrier((kernel_down, ends))
    kernel_down = pltpu.with_memory_space_constraint(kernel_down, pltpu.HBM)
    line = whole((frames, half, c_out), F32)
    edge = whole((cached + 2 * frames, half, c_out), BF16)
    message = whole((1, LANES), F32)
    row, part, third, center, sums, below = pl.pallas_call(
        down_kernel,
        name="down",
        out_shape=(
            line,
            line,
            whole((3, 3, c_in, c_out), BF16),
            whole((1, c_out), F32),
            whole((2, c_out), F32),
            edge,
        ),
        in_specs=[HBM] * 4,
        out_specs=(AUTO,) * 6,
        scratch_shapes=[
            pltpu.VMEM(cache_video.shape, BF16),
            pltpu.VMEM(video.shape, BF16),
            pltpu.VMEM((3, 2, 3, c_in, c_out), BF16),
            pltpu.VMEM((cached + frames, rows, half, 2 * c_in), BF16),
            DMA((5,)),
        ],
        compiler_params=limit(24),
        cost_estimate=pl.CostEstimate(flops=2 * 10**9, bytes_accessed=4 * 10**6, transcendentals=0),
    )(cache_video, video, kernel_down, stored_hidden)
    below = lax.ppermute(below, HA, up)
    last, above, stats = pl.pallas_call(
        rim_down_kernel,
        name="rim_down",
        out_shape=(line, edge, message),
        in_specs=[AUTO] * 8,
        out_specs=(AUTO,) * 3,
        scratch_shapes=[
            pltpu.VMEM((cached + frames, width, c_in), BF16),
            pltpu.VMEM((cached + frames, half, 2 * c_in), BF16),
        ],
        compiler_params=limit(16),
    )(near_rim, far_rim, ends, third, part, center, sums, cache_hidden)
    above = lax.ppermute(above, HA, down)
    stats = everyone(stats)
    second, next_cache, stats = run_mix(
        row, last, above, below, ends, stats, gain_down[None], shift_down[None], cache_hidden, kernel_mix
    )
    stats = everyone(stats)
    encoded = pl.pallas_call(
        final_kernel,
        name="final",
        out_shape=whole((frames, 2, half, c_out), BF16),
        in_specs=[AUTO] * 4,
        out_specs=ANY,
        scratch_shapes=[pltpu.VMEM((frames, 2, half, c_out), BF16), DMA((2 * frames,))],
        compiler_params=limit(8),
    )(second, stats, gain_mix[None], shift_mix[None])
    return (encoded, next_cache)


def solution(mesh):
    split = Mesh(
        mesh.devices.reshape(mesh.shape["groups"], 8, 8, 2), ("groups", "ha_0", "ha_1", "ha_2")
    )
    strips = P("groups", HA, None, None)

    return jax.shard_map(
        local,
        mesh=split,
        in_specs=(strips, strips, strips, P(), P(), P(), P(), P(), P()),
        out_specs=(strips, strips),
        check_vma=False,
    )
```

```python
import jax
import jax.numpy as jnp
from jax import lax
from jax.experimental import pallas as pl
from jax.experimental.pallas import tpu as pltpu
from jax.sharding import Mesh
from jax.sharding import PartitionSpec as P

GROUPS = 32
LANES = 128
EPS = 1e-6
HA = ("ha_0", "ha_1", "ha_2")
F32 = jnp.float32
BF16 = jnp.bfloat16
AUTO = pl.BlockSpec()
ANY = pl.BlockSpec(memory_space=pl.ANY)
HBM = pl.BlockSpec(memory_space=pltpu.HBM)
DMA = pltpu.SemaphoreType.DMA


def limit(mib):
    return pltpu.CompilerParams(vmem_limit_bytes=mib * 2**20)


def lanes_of(x):
    return lax.broadcasted_iota(jnp.int32, x.shape, x.ndim - 1)


def turn(x, by):
    return pltpu.roll(x, by % x.shape[-1], x.ndim - 1)


def group_sum(x):
    lane = lanes_of(x)
    step = 1
    while step < x.shape[-1] // GROUPS:
        x = x + jnp.where((lane & step) != 0, turn(x, step), turn(x, -step))
        step *= 2
    return x


def column_sum(block):
    return jnp.sum(block, axis=0, keepdims=True)


def moments_row(center, sums, squares, count):
    members = count * (center.shape[-1] // GROUPS)
    shift = group_sum(sums) * (1.0 / members)
    squares = group_sum(squares) - shift * shift * members
    mean = center + shift
    kind = lanes_of(mean[:, :LANES]) % 4
    low = jnp.where(kind == 0, mean[:, :LANES], squares[:, :LANES])
    high = jnp.where(kind == 2, mean[:, LANES:], squares[:, LANES:])
    return jnp.where(kind < 2, low, high)


def affine(rows, members, gain):
    devices = rows.shape[0]
    total = column_sum(rows)
    center = total * (1.0 / devices)
    off = rows - center
    between = column_sum(off * off) * members
    spread = (total + turn(between, 1)) * (1.0 / (members * devices))
    rate = lax.rsqrt(jnp.maximum(spread, 0.0) + EPS)
    kind = lanes_of(total) % 4

    def fill(value, at):
        value = jnp.where(kind == at, value, 0.0)
        value = value + turn(value, 1 if at % 2 == 0 else -1)
        return value + turn(value, 2 if at < 2 else -2)

    centers = jnp.concatenate([fill(center, 0), fill(center, 2)], axis=1)
    rates = jnp.concatenate([fill(rate, 1), fill(rate, 3)], axis=1)
    return centers, rates * gain


def silu_norm(values, center, factor, offset):
    normed = (values - center) * factor + offset
    return normed / (1.0 + jnp.exp(-normed))


def shift_back(x):
    rows = x.shape[0]
    place = lax.broadcasted_iota(jnp.int32, x.shape, 0)
    return jnp.where(place == rows - 1, 0.0, pltpu.roll(x, rows - 1, 0))


def shift_on(x):
    place = lax.broadcasted_iota(jnp.int32, x.shape, 0)
    return jnp.where(place == 0, 0.0, pltpu.roll(x, 1, 0))


def rim_kernel(cache_ref, video_ref, out_ref, sems):
    cached = cache_ref.shape[0]
    copies = []
    for f in range(out_ref.shape[0]):
        source = cache_ref.at[f, 0] if f < cached else video_ref.at[f - cached, 0]
        copies.append(pltpu.make_async_copy(source, out_ref.at[f], sems.at[f]))
    for c in copies:
        c.start()
    for c in copies:
        c.wait()


def pair_up(source, target, c_in):
    half = target.shape[0]
    target[:, :c_in] = source[pl.ds(0, half, stride=2), :]
    target[:, c_in:] = source[pl.ds(1, half, stride=2), :]


def split_in_two(value):
    coarse = value.astype(BF16)
    return coarse, (value - coarse.astype(F32)).astype(BF16)


def third_row(pairs, third_ref, frames, half, c_in):
    taps = [pairs[a : a + frames].reshape(frames * half, 2 * c_in) for a in range(3)]
    both = jnp.concatenate([third_ref[a, c] for a in range(3) for c in range(2)], axis=0)
    ahead = jnp.concatenate([third_ref[a, 2] for a in range(3)], axis=0)
    here = jnp.dot(jnp.concatenate(taps, axis=1), both, preferred_element_type=F32)
    evens = jnp.concatenate([t[:, :c_in] for t in taps], axis=1)
    after = jnp.dot(evens, ahead, preferred_element_type=F32)
    spans = [slice(t * half, (t + 1) * half) for t in range(frames)]
    return [here[span] + shift_back(after[span]) for span in spans]


def down_kernel(
    cache_ref, video_ref, kernel_ref, hidden_ref,
    row_ref, part_ref, share_ref, third_ref, center_ref, sums_ref, upper_ref, lower_ref,
    cache_buf, video_buf, kernel_buf, pairs_ref, sems,
):
    frames, rows, width, c_in = video_ref.shape
    cached = cache_ref.shape[0]
    half = width // 2
    c_out = kernel_ref.shape[-1]
    loads = [
        pltpu.make_async_copy(cache_ref, cache_buf, sems.at[0]),
        pltpu.make_async_copy(video_ref, video_buf, sems.at[1]),
        pltpu.make_async_copy(kernel_ref.at[:, :2], kernel_buf, sems.at[2]),
        pltpu.make_async_copy(kernel_ref.at[:, 2], third_ref, sems.at[3]),
        pltpu.make_async_copy(hidden_ref.at[:, 0], upper_ref.at[:cached], sems.at[4]),
        pltpu.make_async_copy(hidden_ref.at[:, rows // 2 - 1], lower_ref.at[:cached], sems.at[5]),
    ]
    for c in loads:
        c.start()
    for f in range(cached + frames):
        if f == 0:
            loads[0].wait()
        if f == cached:
            loads[1].wait()
        for r in range(rows):
            source = cache_buf.at[f, r] if f < cached else video_buf.at[f - cached, r]
            pair_up(source, pairs_ref.at[f, r], c_in)
    loads[2].wait()
    loads[3].wait()

    def tap(a, b, c):
        return third_ref[a, c] if b == 2 else kernel_buf[a, b, c]

    for i, depth in ((0, 3), (1, 2)):
        where = [(a, b) for b in range(depth) for a in range(3)]
        taps = [pairs_ref[a : a + frames, 2 * i + b].reshape(frames * half, 2 * c_in) for a, b in where]
        both = jnp.concatenate([tap(a, b, c) for a, b in where for c in range(2)], axis=0)
        ahead = jnp.concatenate([tap(a, b, 2) for a, b in where], axis=0)
        here = jnp.dot(jnp.concatenate(taps, axis=1), both, preferred_element_type=F32)
        evens = jnp.concatenate([t[:, :c_in] for t in taps], axis=1)
        after = jnp.dot(evens, ahead, preferred_element_type=F32)
        for t in range(frames):
            span = slice(t * half, (t + 1) * half)
            block = here[span] + shift_back(after[span])
            target, edge_ref = (row_ref, upper_ref) if i == 0 else (part_ref, lower_ref)
            target[t] = block
            edge_ref[cached + t], edge_ref[cached + frames + t] = split_in_two(block)
    shares = third_row(pairs_ref[:, 0], third_ref, frames, half, c_in)
    for t in range(frames):
        share_ref[t] = shares[t]
    total = sum(column_sum(row_ref[t]) for t in range(frames))
    center = group_sum(total) * (1.0 / (frames * half * (c_out // GROUPS)))
    center_ref[...] = center
    sums_ref[0:1] = total - center * (frames * half)
    sums_ref[1:2] = sum(column_sum((row_ref[t] - center) ** 2) for t in range(frames))
    loads[4].wait()
    loads[5].wait()


def rim_down_kernel(
    near_ref, far_ref, ends_ref, third_ref, part_ref, center_ref, sums_ref,
    last_ref, message_ref,
    rim_ref, pairs_ref,
):
    frames, half, _ = part_ref.shape
    c_in = near_ref.shape[-1]
    odd = ends_ref[2:3, :c_in].astype(BF16)
    for f in range(rim_ref.shape[0]):
        rim_ref[f] = far_ref[f] * odd + near_ref[f] * (1 - odd)
        pair_up(rim_ref.at[f], pairs_ref.at[f], c_in)
    keep = ends_ref[1:2]
    center = center_ref[...]
    sums, squares = sums_ref[0:1], sums_ref[1:2]
    shares = third_row(pairs_ref[...], third_ref, frames, half, c_in)
    for t in range(frames):
        block = part_ref[t] + jnp.where(keep > 0, shares[t], 0.0)
        last_ref[t] = block
        off = block - center
        sums = sums + column_sum(off)
        squares = squares + column_sum(off * off)
    message_ref[...] = moments_row(center, sums, squares, 2 * frames * half)


def unpack(stats_ref):
    both = stats_ref[...][:, 0]
    return jnp.concatenate([both[:, :LANES], both[:, LANES:]], axis=0)


def mix_kernel(
    row_ref, last_ref, share_ref, above_ref, below_ref, ends_ref, stats_ref, gain_ref, shift_ref, hidden_ref, kernel_ref,
    second_ref, next_ref, message_ref,
    rows_ref, sem,
):
    frames, width, channels = row_ref.shape
    cached = hidden_ref.shape[0]
    rows = 2
    count = rows * frames * width
    for f in range(cached):
        for i in range(rows):
            rows_ref[f, 1 + i] = hidden_ref[f, i]
    keep_above, keep_below = ends_ref[0:1], ends_ref[1:2]
    for f in range(cached):
        rows_ref[f, 0] = above_ref[f] * keep_above.astype(BF16)
        rows_ref[f, rows + 1] = below_ref[f] * keep_below.astype(BF16)
    center, factor = affine(unpack(stats_ref), count * (channels // GROUPS), gain_ref[...])
    offset = shift_ref[...]

    def activate(t):
        for at, edge_ref, keep in ((0, above_ref, keep_above), (rows + 1, below_ref, keep_below)):
            value = edge_ref[cached + t].astype(F32) + edge_ref[cached + frames + t].astype(F32)
            if at == 0:
                value = value + share_ref[t]
            hidden = silu_norm(value, center, factor, offset)
            rows_ref[cached + t, at] = jnp.where(keep > 0, hidden, 0.0).astype(BF16)
        rows_ref[cached + t, 1] = silu_norm(row_ref[t], center, factor, offset).astype(BF16)
        rows_ref[cached + t, 2] = silu_norm(last_ref[t], center, factor, offset).astype(BF16)

    step = frames // 2
    for begin in range(0, frames, step):
        if begin == 0:
            for t in range(step):
                activate(t)
        taps = jnp.concatenate(
            [
                rows_ref[begin + a : begin + a + step, b : b + rows].reshape(step * rows * width, channels)
                for a in range(3)
                for b in range(3)
            ],
            axis=1,
        )
        parts = []
        for c in range(3):
            weights = jnp.concatenate([kernel_ref[a, b, c] for a in range(3) for b in range(3)], axis=0)
            parts.append(jnp.dot(taps, weights, preferred_element_type=F32))
        left, here, right = parts
        if begin == 0:
            for t in range(step, frames):
                activate(t)
        blocks = []
        for n in range(step * rows):
            span = slice(n * width, (n + 1) * width)
            t, i = begin + n // rows, n % rows
            block = here[span] + shift_on(left[span]) + shift_back(right[span])
            second_ref[t, i] = block
            blocks.append(block)
        if begin == 0:
            total = sum(column_sum(b) for b in blocks)
            middle = group_sum(total) * (1.0 / (step * rows * width * (channels // GROUPS)))
            sums = total - middle * (step * rows * width)
            blocks = [second_ref[t, i] for t in range(step) for i in range(rows)]
            squares = sum(column_sum((b - middle) ** 2) for b in blocks)
        else:
            offs = [b - middle for b in blocks]
            sums = sums + sum(column_sum(off) for off in offs)
            squares = squares + sum(column_sum(off * off) for off in offs)
    store = pltpu.make_async_copy(
        rows_ref.at[cached + frames - 2 : cached + frames, 1 : 1 + rows], next_ref, sem
    )
    store.start()
    message_ref[...] = moments_row(middle, sums, squares, count)
    store.wait()


def final_kernel(second_ref, stats_ref, gain_ref, shift_ref, out_ref, buf, sems):
    frames, rows, width, channels = second_ref.shape
    members = frames * rows * width * (channels // GROUPS)
    center, factor = affine(unpack(stats_ref), members, gain_ref[...])
    offset = shift_ref[...]
    stores = []
    for t in range(frames):
        for i in range(rows):
            buf[t, i] = silu_norm(second_ref[t, i], center, factor, offset).astype(BF16)
            stores.append(pltpu.make_async_copy(buf.at[t, i], out_ref.at[t, i], sems.at[t * rows + i]))
            stores[-1].start()
    for c in stores:
        c.wait()


def both_kernel(mine_ref, other_ref, out_ref):
    both = jnp.concatenate([mine_ref[...], other_ref[...]], axis=1)
    out_ref[...] = jnp.broadcast_to(both[None], out_ref.shape)


def everyone(message):
    devices, chips = lax.axis_size(HA), lax.axis_size(HA[:-1])
    other = lax.ppermute(message, HA, [(i, i ^ 1) for i in range(devices)])
    copies = pl.pallas_call(
        both_kernel,
        name="both",
        out_shape=jax.ShapeDtypeStruct((chips, 1, 2 * LANES), F32),
        in_specs=[AUTO] * 2,
        out_specs=AUTO,
        compiler_params=limit(1),
    )(message, other)
    return lax.all_to_all(copies, HA[:-1], 0, 0)


def run_mix(row, last, share, above, below, ends, stats, gain, shift, hidden, kernel):
    frames, half, c_out = row.shape
    cached = hidden.shape[0]
    whole = jax.ShapeDtypeStruct
    return pl.pallas_call(
        mix_kernel,
        name="mix",
        out_shape=(
            whole((frames, 2, half, c_out), F32),
            whole((2, 2, half, c_out), BF16),
            whole((1, LANES), F32),
        ),
        in_specs=[AUTO] * 11,
        out_specs=(AUTO, ANY, AUTO),
        scratch_shapes=[pltpu.VMEM((cached + frames, 4, half, c_out), BF16), DMA(())],
        compiler_params=limit(28),
    )(row, last, share, above, below, ends, stats, gain, shift, hidden, kernel)


def local(video, cache_video, cache_hidden, kernel_down, gain_down, shift_down, kernel_mix, gain_mix, shift_mix):
    frames, rows, width, c_in = video.shape
    cached = cache_video.shape[0]
    c_out = kernel_down.shape[-1]
    half = width // 2
    video, cache_video, stored_hidden = (
        pltpu.with_memory_space_constraint(x, pltpu.HBM) for x in (video, cache_video, cache_hidden)
    )
    devices = lax.axis_size(HA)
    place = lax.axis_index(HA)
    up = [((i + 1) % devices, i) for i in range(devices)]
    down = [(i, (i + 1) % devices) for i in range(devices)]
    whole = jax.ShapeDtypeStruct
    rim = pl.pallas_call(
        rim_kernel,
        name="rim",
        out_shape=whole((cached + frames, width, c_in), BF16),
        in_specs=[HBM] * 2,
        out_specs=AUTO,
        scratch_shapes=[DMA((cached + frames,))],
        compiler_params=limit(4),
    )(cache_video, video)
    pairs = [(i, i ^ 1) for i in range(devices)]
    bridges = [(i, min(max(i + (1 if i % 2 else -1), 0), devices - 1)) for i in range(devices)]
    near_rim = lax.ppermute(rim, HA, pairs)
    far_rim = lax.ppermute(rim, HA, bridges)
    ends = jnp.broadcast_to(
        jnp.stack([place > 0, place < devices - 1, place % 2 > 0]).astype(F32)[:, None], (3, c_out)
    )
    kernel_down, ends = lax.optimization_barrier((kernel_down, ends))
    kernel_down = pltpu.with_memory_space_constraint(kernel_down, pltpu.HBM)
    line = whole((frames, half, c_out), F32)
    edge = whole((cached + 2 * frames, half, c_out), BF16)
    message = whole((1, LANES), F32)
    row, part, share, third, center, sums, below, above = pl.pallas_call(
        down_kernel,
        name="down",
        out_shape=(
            line,
            line,
            line,
            whole((3, 3, c_in, c_out), BF16),
            whole((1, c_out), F32),
            whole((2, c_out), F32),
            edge,
            edge,
        ),
        in_specs=[HBM] * 4,
        out_specs=(AUTO,) * 8,
        scratch_shapes=[
            pltpu.VMEM(cache_video.shape, BF16),
            pltpu.VMEM(video.shape, BF16),
            pltpu.VMEM((3, 2, 3, c_in, c_out), BF16),
            pltpu.VMEM((cached + frames, rows, half, 2 * c_in), BF16),
            DMA((6,)),
        ],
        compiler_params=limit(24),
        cost_estimate=pl.CostEstimate(flops=2 * 10**9, bytes_accessed=4 * 10**6, transcendentals=0),
    )(cache_video, video, kernel_down, stored_hidden)
    below = lax.ppermute(below, HA, up)
    above = lax.ppermute(above, HA, down)
    last, stats = pl.pallas_call(
        rim_down_kernel,
        name="rim_down",
        out_shape=(line, message),
        in_specs=[AUTO] * 7,
        out_specs=(AUTO,) * 2,
        scratch_shapes=[
            pltpu.VMEM((cached + frames, width, c_in), BF16),
            pltpu.VMEM((cached + frames, half, 2 * c_in), BF16),
        ],
        compiler_params=limit(16),
    )(near_rim, far_rim, ends, third, part, center, sums)
    stats = everyone(stats)
    second, next_cache, stats = run_mix(
        row, last, share, above, below, ends, stats, gain_down[None], shift_down[None], cache_hidden, kernel_mix
    )
    stats = everyone(stats)
    encoded = pl.pallas_call(
        final_kernel,
        name="final",
        out_shape=whole((frames, 2, half, c_out), BF16),
        in_specs=[AUTO] * 4,
        out_specs=ANY,
        scratch_shapes=[pltpu.VMEM((frames, 2, half, c_out), BF16), DMA((2 * frames,))],
        compiler_params=limit(8),
    )(second, stats, gain_mix[None], shift_mix[None])
    return (encoded, next_cache)


def solution(mesh):
    split = Mesh(
        mesh.devices.reshape(mesh.shape["groups"], 8, 8, 2), ("groups", "ha_0", "ha_1", "ha_2")
    )
    strips = P("groups", HA, None, None)

    return jax.shard_map(
        local,
        mesh=split,
        in_specs=(strips, strips, strips, P(), P(), P(), P(), P(), P()),
        out_specs=(strips, strips),
        check_vma=False,
    )
```

```python
import jax
import jax.numpy as jnp
from jax import lax
from jax.experimental import pallas as pl
from jax.experimental.pallas import tpu as pltpu
from jax.sharding import Mesh
from jax.sharding import PartitionSpec as P

GROUPS = 32
LANES = 128
EPS = 1e-6
HA = ("ha_0", "ha_1", "ha_2")
F32 = jnp.float32
BF16 = jnp.bfloat16
AUTO = pl.BlockSpec()
ANY = pl.BlockSpec(memory_space=pl.ANY)
HBM = pl.BlockSpec(memory_space=pltpu.HBM)
DMA = pltpu.SemaphoreType.DMA


def limit(mib):
    return pltpu.CompilerParams(vmem_limit_bytes=mib * 2**20)


def lanes_of(x):
    return lax.broadcasted_iota(jnp.int32, x.shape, x.ndim - 1)


def turn(x, by):
    return pltpu.roll(x, by % x.shape[-1], x.ndim - 1)


def group_sum(x):
    lane = lanes_of(x)
    step = 1
    while step < x.shape[-1] // GROUPS:
        x = x + jnp.where((lane & step) != 0, turn(x, step), turn(x, -step))
        step *= 2
    return x


def column_sum(block):
    return jnp.sum(block, axis=0, keepdims=True)


def moments_row(center, sums, squares, count):
    members = count * (center.shape[-1] // GROUPS)
    shift = group_sum(sums) * (1.0 / members)
    squares = group_sum(squares) - shift * shift * members
    mean = center + shift
    kind = lanes_of(mean[:, :LANES]) % 4
    low = jnp.where(kind == 0, mean[:, :LANES], squares[:, :LANES])
    high = jnp.where(kind == 2, mean[:, LANES:], squares[:, LANES:])
    return jnp.where(kind < 2, low, high)


def affine(rows, members, gain):
    devices = rows.shape[0]
    total = column_sum(rows)
    center = total * (1.0 / devices)
    off = rows - center
    between = column_sum(off * off) * members
    spread = (total + turn(between, 1)) * (1.0 / (members * devices))
    rate = lax.rsqrt(jnp.maximum(spread, 0.0) + EPS)
    kind = lanes_of(total) % 4

    def fill(value, at):
        value = jnp.where(kind == at, value, 0.0)
        value = value + turn(value, 1 if at % 2 == 0 else -1)
        return value + turn(value, 2 if at < 2 else -2)

    centers = jnp.concatenate([fill(center, 0), fill(center, 2)], axis=1)
    rates = jnp.concatenate([fill(rate, 1), fill(rate, 3)], axis=1)
    return centers, rates * gain


def silu_norm(values, center, factor, offset):
    normed = (values - center) * factor + offset
    return normed / (1.0 + jnp.exp(-normed))


def shift_back(x):
    rows = x.shape[0]
    place = lax.broadcasted_iota(jnp.int32, x.shape, 0)
    return jnp.where(place == rows - 1, 0.0, pltpu.roll(x, rows - 1, 0))


def shift_on(x):
    place = lax.broadcasted_iota(jnp.int32, x.shape, 0)
    return jnp.where(place == 0, 0.0, pltpu.roll(x, 1, 0))


def rim_kernel(cache_ref, video_ref, out_ref, sems):
    cached = cache_ref.shape[0]
    copies = []
    for f in range(out_ref.shape[0]):
        source = cache_ref.at[f, 0] if f < cached else video_ref.at[f - cached, 0]
        copies.append(pltpu.make_async_copy(source, out_ref.at[f], sems.at[f]))
    for c in copies:
        c.start()
    for c in copies:
        c.wait()


def pair_up(source, target, c_in):
    half = target.shape[0]
    target[:, :c_in] = source[pl.ds(0, half, stride=2), :]
    target[:, c_in:] = source[pl.ds(1, half, stride=2), :]


def split_in_two(value):
    coarse = value.astype(BF16)
    return coarse, (value - coarse.astype(F32)).astype(BF16)


def third_row(pairs, third_ref, frames, half, c_in):
    taps = [pairs[a : a + frames].reshape(frames * half, 2 * c_in) for a in range(3)]
    both = jnp.concatenate([third_ref[a, c] for a in range(3) for c in range(2)], axis=0)
    ahead = jnp.concatenate([third_ref[a, 2] for a in range(3)], axis=0)
    here = jnp.dot(jnp.concatenate(taps, axis=1), both, preferred_element_type=F32)
    evens = jnp.concatenate([t[:, :c_in] for t in taps], axis=1)
    after = jnp.dot(evens, ahead, preferred_element_type=F32)
    spans = [slice(t * half, (t + 1) * half) for t in range(frames)]
    return [here[span] + shift_back(after[span]) for span in spans]


def down_kernel(
    ends_ref, cache_ref, video_ref, kernel_ref, hidden_ref,
    row_ref, part_ref, share_ref, third_ref, center_ref, sums_ref, near_ref, far_ref,
    hidden_buf, cache_buf, video_buf, kernel_buf, pairs_ref, sems,
):
    frames, rows, width, c_in = video_ref.shape
    cached = cache_ref.shape[0]
    half = width // 2
    c_out = kernel_ref.shape[-1]
    loads = [
        pltpu.make_async_copy(cache_ref, cache_buf, sems.at[0]),
        pltpu.make_async_copy(video_ref, video_buf, sems.at[1]),
        pltpu.make_async_copy(kernel_ref.at[:, :2], kernel_buf, sems.at[2]),
        pltpu.make_async_copy(kernel_ref.at[:, 2], third_ref, sems.at[3]),
        pltpu.make_async_copy(hidden_ref, hidden_buf, sems.at[4]),
    ]
    for c in loads:
        c.start()
    for f in range(cached + frames):
        if f == 0:
            loads[0].wait()
        if f == cached:
            loads[1].wait()
        for r in range(rows):
            source = cache_buf.at[f, r] if f < cached else video_buf.at[f - cached, r]
            pair_up(source, pairs_ref.at[f, r], c_in)
    loads[2].wait()
    loads[3].wait()

    odd = ends_ref[2:3]

    def tap(a, b, c):
        return third_ref[a, c] if b == 2 else kernel_buf[a, b, c]

    for i, depth in ((0, 3), (1, 2)):
        where = [(a, b) for b in range(depth) for a in range(3)]
        taps = [pairs_ref[a : a + frames, 2 * i + b].reshape(frames * half, 2 * c_in) for a, b in where]
        both = jnp.concatenate([tap(a, b, c) for a, b in where for c in range(2)], axis=0)
        ahead = jnp.concatenate([tap(a, b, 2) for a, b in where], axis=0)
        here = jnp.dot(jnp.concatenate(taps, axis=1), both, preferred_element_type=F32)
        evens = jnp.concatenate([t[:, :c_in] for t in taps], axis=1)
        after = jnp.dot(evens, ahead, preferred_element_type=F32)
        for t in range(frames):
            span = slice(t * half, (t + 1) * half)
            block = here[span] + shift_back(after[span])
            if i == 0:
                row_ref[t] = block
            else:
                part_ref[t] = block
                upper = row_ref[t]
                for edge_ref, edge in (
                    (near_ref, jnp.where(odd > 0, upper, block)),
                    (far_ref, jnp.where(odd > 0, block, upper)),
                ):
                    edge_ref[cached + t], edge_ref[cached + frames + t] = split_in_two(edge)
    shares = third_row(pairs_ref[:, 0], third_ref, frames, half, c_in)
    for t in range(frames):
        share_ref[t] = shares[t]
    total = sum(column_sum(row_ref[t]) for t in range(frames))
    center = group_sum(total) * (1.0 / (frames * half * (c_out // GROUPS)))
    center_ref[...] = center
    sums_ref[0:1] = total - center * (frames * half)
    sums_ref[1:2] = sum(column_sum((row_ref[t] - center) ** 2) for t in range(frames))
    loads[4].wait()
    odd_bits = odd.astype(BF16)
    for f in range(cached):
        upper, lower = hidden_buf[f, 0], hidden_buf[f, rows // 2 - 1]
        near_ref[f] = upper * odd_bits + lower * (1 - odd_bits)
        far_ref[f] = lower * odd_bits + upper * (1 - odd_bits)


def rim_down_kernel(
    near_ref, far_ref, ends_ref, third_ref, part_ref, center_ref, sums_ref,
    last_ref, message_ref,
    rim_ref, pairs_ref,
):
    frames, half, _ = part_ref.shape
    c_in = near_ref.shape[-1]
    odd = ends_ref[2:3, :c_in].astype(BF16)
    for f in range(rim_ref.shape[0]):
        rim_ref[f] = far_ref[f] * odd + near_ref[f] * (1 - odd)
        pair_up(rim_ref.at[f], pairs_ref.at[f], c_in)
    keep = ends_ref[1:2]
    center = center_ref[...]
    sums, squares = sums_ref[0:1], sums_ref[1:2]
    shares = third_row(pairs_ref[...], third_ref, frames, half, c_in)
    for t in range(frames):
        block = part_ref[t] + jnp.where(keep > 0, shares[t], 0.0)
        last_ref[t] = block
        off = block - center
        sums = sums + column_sum(off)
        squares = squares + column_sum(off * off)
    message_ref[...] = moments_row(center, sums, squares, 2 * frames * half)


def unpack(stats_ref):
    both = stats_ref[...][:, 0]
    return jnp.concatenate([both[:, :LANES], both[:, LANES:]], axis=0)


def mix_kernel(
    row_ref, last_ref, share_ref, near_ref, far_ref, ends_ref, stats_ref, gain_ref, shift_ref, hidden_ref, kernel_ref,
    second_ref, next_ref, message_ref,
    rows_ref, sem,
):
    frames, width, channels = row_ref.shape
    cached = hidden_ref.shape[0]
    rows = 2
    count = rows * frames * width
    for f in range(cached):
        for i in range(rows):
            rows_ref[f, 1 + i] = hidden_ref[f, i]
    keep_above, keep_below = ends_ref[0:1], ends_ref[1:2]
    odd = ends_ref[2:3]
    for at, keep, is_near in ((0, keep_above, odd), (rows + 1, keep_below, 1.0 - odd)):
        near_share = (keep * is_near).astype(BF16)
        far_share = (keep * (1.0 - is_near)).astype(BF16)
        for f in range(cached):
            rows_ref[f, at] = near_ref[f] * near_share + far_ref[f] * far_share
    center, factor = affine(unpack(stats_ref), count * (channels // GROUPS), gain_ref[...])
    offset = shift_ref[...]

    def activate(t):
        near, far = (
            ref[cached + t].astype(F32) + ref[cached + frames + t].astype(F32) for ref in (near_ref, far_ref)
        )
        above = jnp.where(odd > 0, near, far) + share_ref[t]
        below = jnp.where(odd > 0, far, near)
        for at, value, keep in ((0, above, keep_above), (rows + 1, below, keep_below)):
            hidden = silu_norm(value, center, factor, offset)
            rows_ref[cached + t, at] = jnp.where(keep > 0, hidden, 0.0).astype(BF16)
        rows_ref[cached + t, 1] = silu_norm(row_ref[t], center, factor, offset).astype(BF16)
        rows_ref[cached + t, 2] = silu_norm(last_ref[t], center, factor, offset).astype(BF16)

    step = frames // 2
    for begin in range(0, frames, step):
        if begin == 0:
            for t in range(step):
                activate(t)
        taps = jnp.concatenate(
            [
                rows_ref[begin + a : begin + a + step, b : b + rows].reshape(step * rows * width, channels)
                for a in range(3)
                for b in range(3)
            ],
            axis=1,
        )
        parts = []
        for c in range(3):
            weights = jnp.concatenate([kernel_ref[a, b, c] for a in range(3) for b in range(3)], axis=0)
            parts.append(jnp.dot(taps, weights, preferred_element_type=F32))
        left, here, right = parts
        if begin == 0:
            for t in range(step, frames):
                activate(t)
        blocks = []
        for n in range(step * rows):
            span = slice(n * width, (n + 1) * width)
            t, i = begin + n // rows, n % rows
            block = here[span] + shift_on(left[span]) + shift_back(right[span])
            second_ref[t, i] = block
            blocks.append(block)
        if begin == 0:
            total = sum(column_sum(b) for b in blocks)
            middle = group_sum(total) * (1.0 / (step * rows * width * (channels // GROUPS)))
            sums = total - middle * (step * rows * width)
            blocks = [second_ref[t, i] for t in range(step) for i in range(rows)]
            squares = sum(column_sum((b - middle) ** 2) for b in blocks)
        else:
            offs = [b - middle for b in blocks]
            sums = sums + sum(column_sum(off) for off in offs)
            squares = squares + sum(column_sum(off * off) for off in offs)
    store = pltpu.make_async_copy(
        rows_ref.at[cached + frames - 2 : cached + frames, 1 : 1 + rows], next_ref, sem
    )
    store.start()
    message_ref[...] = moments_row(middle, sums, squares, count)
    store.wait()


def final_kernel(second_ref, stats_ref, gain_ref, shift_ref, out_ref, buf, sems):
    frames, rows, width, channels = second_ref.shape
    members = frames * rows * width * (channels // GROUPS)
    center, factor = affine(unpack(stats_ref), members, gain_ref[...])
    offset = shift_ref[...]
    stores = []
    for t in range(frames):
        for i in range(rows):
            buf[t, i] = silu_norm(second_ref[t, i], center, factor, offset).astype(BF16)
            stores.append(pltpu.make_async_copy(buf.at[t, i], out_ref.at[t, i], sems.at[t * rows + i]))
            stores[-1].start()
    for c in stores:
        c.wait()


def both_kernel(mine_ref, other_ref, out_ref):
    both = jnp.concatenate([mine_ref[...], other_ref[...]], axis=1)
    out_ref[...] = jnp.broadcast_to(both[None], out_ref.shape)


def everyone(message):
    devices, chips = lax.axis_size(HA), lax.axis_size(HA[:-1])
    other = lax.ppermute(message, HA, [(i, i ^ 1) for i in range(devices)])
    copies = pl.pallas_call(
        both_kernel,
        name="both",
        out_shape=jax.ShapeDtypeStruct((chips, 1, 2 * LANES), F32),
        in_specs=[AUTO] * 2,
        out_specs=AUTO,
        compiler_params=limit(1),
    )(message, other)
    return lax.all_to_all(copies, HA[:-1], 0, 0)


def run_mix(row, last, share, near, far, ends, stats, gain, shift, hidden, kernel):
    frames, half, c_out = row.shape
    cached = hidden.shape[0]
    whole = jax.ShapeDtypeStruct
    return pl.pallas_call(
        mix_kernel,
        name="mix",
        out_shape=(
            whole((frames, 2, half, c_out), F32),
            whole((2, 2, half, c_out), BF16),
            whole((1, LANES), F32),
        ),
        in_specs=[AUTO] * 11,
        out_specs=(AUTO, ANY, AUTO),
        scratch_shapes=[pltpu.VMEM((cached + frames, 4, half, c_out), BF16), DMA(())],
        compiler_params=limit(28),
    )(row, last, share, near, far, ends, stats, gain, shift, hidden, kernel)


def local(video, cache_video, cache_hidden, kernel_down, gain_down, shift_down, kernel_mix, gain_mix, shift_mix):
    frames, rows, width, c_in = video.shape
    cached = cache_video.shape[0]
    c_out = kernel_down.shape[-1]
    half = width // 2
    video, cache_video, stored_hidden = (
        pltpu.with_memory_space_constraint(x, pltpu.HBM) for x in (video, cache_video, cache_hidden)
    )
    devices = lax.axis_size(HA)
    place = lax.axis_index(HA)
    whole = jax.ShapeDtypeStruct
    rim = pl.pallas_call(
        rim_kernel,
        name="rim",
        out_shape=whole((cached + frames, width, c_in), BF16),
        in_specs=[HBM] * 2,
        out_specs=AUTO,
        scratch_shapes=[DMA((cached + frames,))],
        compiler_params=limit(4),
    )(cache_video, video)
    pairs = [(i, i ^ 1) for i in range(devices)]
    bridges = [(i, min(max(i + (1 if i % 2 else -1), 0), devices - 1)) for i in range(devices)]
    near_rim = lax.ppermute(rim, HA, pairs)
    far_rim = lax.ppermute(rim, HA, bridges)
    ends = jnp.broadcast_to(
        jnp.stack([place > 0, place < devices - 1, place % 2 > 0]).astype(F32)[:, None], (3, c_out)
    )
    kernel_down, ends = lax.optimization_barrier((kernel_down, ends))
    kernel_down = pltpu.with_memory_space_constraint(kernel_down, pltpu.HBM)
    line = whole((frames, half, c_out), F32)
    edge = whole((cached + 2 * frames, half, c_out), BF16)
    message = whole((1, LANES), F32)
    row, part, share, third, center, sums, near_edge, far_edge = pl.pallas_call(
        down_kernel,
        name="down",
        out_shape=(
            line,
            line,
            line,
            whole((3, 3, c_in, c_out), BF16),
            whole((1, c_out), F32),
            whole((2, c_out), F32),
            edge,
            edge,
        ),
        in_specs=[AUTO] + [HBM] * 4,
        out_specs=(AUTO,) * 8,
        scratch_shapes=[
            pltpu.VMEM(cache_hidden.shape, BF16),
            pltpu.VMEM(cache_video.shape, BF16),
            pltpu.VMEM(video.shape, BF16),
            pltpu.VMEM((3, 2, 3, c_in, c_out), BF16),
            pltpu.VMEM((cached + frames, rows, half, 2 * c_in), BF16),
            DMA((5,)),
        ],
        compiler_params=limit(24),
        cost_estimate=pl.CostEstimate(flops=2 * 10**9, bytes_accessed=4 * 10**6, transcendentals=0),
    )(ends, cache_video, video, kernel_down, stored_hidden)
    far_edge = lax.ppermute(far_edge, HA, bridges)
    near_edge = lax.ppermute(near_edge, HA, pairs)
    last, stats = pl.pallas_call(
        rim_down_kernel,
        name="rim_down",
        out_shape=(line, message),
        in_specs=[AUTO] * 7,
        out_specs=(AUTO,) * 2,
        scratch_shapes=[
            pltpu.VMEM((cached + frames, width, c_in), BF16),
            pltpu.VMEM((cached + frames, half, 2 * c_in), BF16),
        ],
        compiler_params=limit(16),
    )(near_rim, far_rim, ends, third, part, center, sums)
    stats = everyone(stats)
    second, next_cache, stats = run_mix(
        row, last, share, near_edge, far_edge, ends, stats, gain_down[None], shift_down[None], cache_hidden, kernel_mix
    )
    stats = everyone(stats)
    encoded = pl.pallas_call(
        final_kernel,
        name="final",
        out_shape=whole((frames, 2, half, c_out), BF16),
        in_specs=[AUTO] * 4,
        out_specs=ANY,
        scratch_shapes=[pltpu.VMEM((frames, 2, half, c_out), BF16), DMA((2 * frames,))],
        compiler_params=limit(8),
    )(second, stats, gain_mix[None], shift_mix[None])
    return (encoded, next_cache)


def solution(mesh):
    split = Mesh(
        mesh.devices.reshape(mesh.shape["groups"], 8, 8, 2), ("groups", "ha_0", "ha_1", "ha_2")
    )
    strips = P("groups", HA, None, None)

    return jax.shard_map(
        local,
        mesh=split,
        in_specs=(strips, strips, strips, P(), P(), P(), P(), P(), P()),
        out_specs=(strips, strips),
        check_vma=False,
    )
```

```python
import jax
import jax.numpy as jnp
from jax import lax
from jax.experimental import pallas as pl
from jax.experimental.pallas import tpu as pltpu
from jax.sharding import Mesh
from jax.sharding import PartitionSpec as P

GROUPS = 32
LANES = 128
EPS = 1e-6
HA = ("ha_0", "ha_1", "ha_2")
F32 = jnp.float32
BF16 = jnp.bfloat16
AUTO = pl.BlockSpec()
ANY = pl.BlockSpec(memory_space=pl.ANY)
HBM = pl.BlockSpec(memory_space=pltpu.HBM)
DMA = pltpu.SemaphoreType.DMA


def limit(mib):
    return pltpu.CompilerParams(vmem_limit_bytes=mib * 2**20)


def lanes_of(x):
    return lax.broadcasted_iota(jnp.int32, x.shape, x.ndim - 1)


def turn(x, by):
    return pltpu.roll(x, by % x.shape[-1], x.ndim - 1)


def group_sum(x):
    lane = lanes_of(x)
    step = 1
    while step < x.shape[-1] // GROUPS:
        x = x + jnp.where((lane & step) != 0, turn(x, step), turn(x, -step))
        step *= 2
    return x


def column_sum(block):
    return jnp.sum(block, axis=0, keepdims=True)


def moments_row(center, sums, squares, count):
    members = count * (center.shape[-1] // GROUPS)
    shift = group_sum(sums) * (1.0 / members)
    squares = group_sum(squares) - shift * shift * members
    mean = center + shift
    kind = lanes_of(mean[:, :LANES]) % 4
    low = jnp.where(kind == 0, mean[:, :LANES], squares[:, :LANES])
    high = jnp.where(kind == 2, mean[:, LANES:], squares[:, LANES:])
    return jnp.where(kind < 2, low, high)


def affine(rows, members, gain):
    devices = rows.shape[0]
    total = column_sum(rows)
    center = total * (1.0 / devices)
    off = rows - center
    between = column_sum(off * off) * members
    spread = (total + turn(between, 1)) * (1.0 / (members * devices))
    rate = lax.rsqrt(jnp.maximum(spread, 0.0) + EPS)
    kind = lanes_of(total) % 4

    def fill(value, at):
        value = jnp.where(kind == at, value, 0.0)
        value = value + turn(value, 1 if at % 2 == 0 else -1)
        return value + turn(value, 2 if at < 2 else -2)

    centers = jnp.concatenate([fill(center, 0), fill(center, 2)], axis=1)
    rates = jnp.concatenate([fill(rate, 1), fill(rate, 3)], axis=1)
    return centers, rates * gain


def silu_norm(values, center, factor, offset):
    normed = (values - center) * factor + offset
    return normed / (1.0 + jnp.exp(-normed))


def shift_back(x):
    rows = x.shape[0]
    place = lax.broadcasted_iota(jnp.int32, x.shape, 0)
    return jnp.where(place == rows - 1, 0.0, pltpu.roll(x, rows - 1, 0))


def shift_on(x):
    place = lax.broadcasted_iota(jnp.int32, x.shape, 0)
    return jnp.where(place == 0, 0.0, pltpu.roll(x, 1, 0))


def rim_kernel(cache_ref, video_ref, out_ref, ends_ref, sems):
    cached = cache_ref.shape[0]
    copies = []
    for f in range(out_ref.shape[0]):
        source = cache_ref.at[f, 0] if f < cached else video_ref.at[f - cached, 0]
        copies.append(pltpu.make_async_copy(source, out_ref.at[f], sems.at[f]))
    for c in copies:
        c.start()
    place = lax.axis_index(HA)
    flags = (place > 0, place < lax.axis_size(HA) - 1, place % 2 > 0)
    for n, flag in enumerate(flags):
        ends_ref[n : n + 1] = jnp.full((1, ends_ref.shape[1]), jnp.where(flag, 1.0, 0.0), F32)
    for c in copies:
        c.wait()


def pair_up(source, target, c_in):
    half = target.shape[0]
    target[:, :c_in] = source[pl.ds(0, half, stride=2), :]
    target[:, c_in:] = source[pl.ds(1, half, stride=2), :]


def split_in_two(value):
    coarse = value.astype(BF16)
    return coarse, (value - coarse.astype(F32)).astype(BF16)


def down_kernel(
    cache_ref, video_ref, kernel_ref, hidden_ref,
    row_ref, part_ref, third_ref, center_ref, sums_ref, edge_ref,
    cache_buf, video_buf, kernel_buf, pairs_ref, sems,
):
    frames, rows, width, c_in = video_ref.shape
    cached = cache_ref.shape[0]
    half = width // 2
    c_out = kernel_ref.shape[-1]
    loads = [
        pltpu.make_async_copy(cache_ref, cache_buf, sems.at[0]),
        pltpu.make_async_copy(video_ref, video_buf, sems.at[1]),
        pltpu.make_async_copy(kernel_ref.at[:, :2], kernel_buf, sems.at[2]),
        pltpu.make_async_copy(kernel_ref.at[:, 2], third_ref, sems.at[3]),
        pltpu.make_async_copy(hidden_ref.at[:, 0], edge_ref.at[:cached], sems.at[4]),
    ]
    loads[0].start()
    loads[1].start()
    for f in range(cached + frames):
        if f == 0:
            loads[0].wait()
            for c in loads[2:]:
                c.start()
        if f == cached:
            loads[1].wait()
        for r in range(rows):
            source = cache_buf.at[f, r] if f < cached else video_buf.at[f - cached, r]
            pair_up(source, pairs_ref.at[f, r], c_in)
    loads[2].wait()
    loads[3].wait()

    def tap(a, b, c):
        return third_ref[a, c] if b == 2 else kernel_buf[a, b, c]

    for i, depth in ((0, 3), (1, 2)):
        where = [(a, b) for b in range(depth) for a in range(3)]
        taps = [pairs_ref[a : a + frames, 2 * i + b].reshape(frames * half, 2 * c_in) for a, b in where]
        both = jnp.concatenate([tap(a, b, c) for a, b in where for c in range(2)], axis=0)
        ahead = jnp.concatenate([tap(a, b, 2) for a, b in where], axis=0)
        here = jnp.dot(jnp.concatenate(taps, axis=1), both, preferred_element_type=F32)
        evens = jnp.concatenate([t[:, :c_in] for t in taps], axis=1)
        after = jnp.dot(evens, ahead, preferred_element_type=F32)
        for t in range(frames):
            span = slice(t * half, (t + 1) * half)
            block = here[span] + shift_back(after[span])
            if i == 0:
                row_ref[t] = block
                edge_ref[cached + t], edge_ref[cached + frames + t] = split_in_two(block)
            else:
                part_ref[t] = block
    total = sum(column_sum(row_ref[t]) for t in range(frames))
    center = group_sum(total) * (1.0 / (frames * half * (c_out // GROUPS)))
    center_ref[...] = center
    sums_ref[0:1] = total - center * (frames * half)
    sums_ref[1:2] = sum(column_sum((row_ref[t] - center) ** 2) for t in range(frames))
    loads[4].wait()


def rim_down_kernel(
    near_ref, far_ref, ends_ref, third_ref, part_ref, center_ref, sums_ref, hidden_ref,
    last_ref, edge_ref, message_ref,
    rim_ref, pairs_ref,
):
    frames, half, _ = part_ref.shape
    c_in = near_ref.shape[-1]
    cached, rows = hidden_ref.shape[:2]
    for f in range(cached):
        edge_ref[f] = hidden_ref[f, rows - 1]
    odd = ends_ref[2:3, :c_in].astype(BF16)
    for f in range(rim_ref.shape[0]):
        rim_ref[f] = far_ref[f] * odd + near_ref[f] * (1 - odd)
        pair_up(rim_ref.at[f], pairs_ref.at[f], c_in)
    taps = [pairs_ref[a : a + frames].reshape(frames * half, 2 * c_in) for a in range(3)]
    both = jnp.concatenate([third_ref[a, c] for a in range(3) for c in range(2)], axis=0)
    ahead = jnp.concatenate([third_ref[a, 2] for a in range(3)], axis=0)
    here = jnp.dot(jnp.concatenate(taps, axis=1), both, preferred_element_type=F32)
    evens = jnp.concatenate([t[:, :c_in] for t in taps], axis=1)
    after = jnp.dot(evens, ahead, preferred_element_type=F32)
    keep = ends_ref[1:2]
    center = center_ref[...]
    sums, squares = sums_ref[0:1], sums_ref[1:2]
    for t in range(frames):
        span = slice(t * half, (t + 1) * half)
        block = part_ref[t] + jnp.where(keep > 0, here[span] + shift_back(after[span]), 0.0)
        last_ref[t] = block
        edge_ref[cached + t], edge_ref[cached + frames + t] = split_in_two(block)
        off = block - center
        sums = sums + column_sum(off)
        squares = squares + column_sum(off * off)
    message_ref[...] = moments_row(center, sums, squares, 2 * frames * half)


def unpack(stats_ref):
    both = stats_ref[...][:, 0]
    return jnp.concatenate([both[:, :LANES], both[:, LANES:]], axis=0)


def mix_kernel(
    row_ref, last_ref, above_ref, below_ref, ends_ref, stats_ref, gain_ref, shift_ref, hidden_ref, kernel_ref,
    second_ref, next_ref, message_ref,
    rows_ref, sem,
):
    frames, width, channels = row_ref.shape
    cached = hidden_ref.shape[0]
    rows = 2
    count = rows * frames * width
    for f in range(cached):
        for i in range(rows):
            rows_ref[f, 1 + i] = hidden_ref[f, i]
    keep_above, keep_below = ends_ref[0:1], ends_ref[1:2]
    for f in range(cached):
        rows_ref[f, 0] = above_ref[f] * keep_above.astype(BF16)
        rows_ref[f, rows + 1] = below_ref[f] * keep_below.astype(BF16)
    center, factor = affine(unpack(stats_ref), count * (channels // GROUPS), gain_ref[...])
    offset = shift_ref[...]

    def activate(t):
        for at, edge_ref, keep in ((0, above_ref, keep_above), (rows + 1, below_ref, keep_below)):
            value = edge_ref[cached + t].astype(F32) + edge_ref[cached + frames + t].astype(F32)
            hidden = silu_norm(value, center, factor, offset)
            rows_ref[cached + t, at] = jnp.where(keep > 0, hidden, 0.0).astype(BF16)
        rows_ref[cached + t, 1] = silu_norm(row_ref[t], center, factor, offset).astype(BF16)
        rows_ref[cached + t, 2] = silu_norm(last_ref[t], center, factor, offset).astype(BF16)

    step = frames // 2
    for begin in range(0, frames, step):
        if begin == 0:
            for t in range(step):
                activate(t)
        taps = jnp.concatenate(
            [
                rows_ref[begin + a : begin + a + step, b : b + rows].reshape(step * rows * width, channels)
                for a in range(3)
                for b in range(3)
            ],
            axis=1,
        )
        parts = []
        for c in range(3):
            weights = jnp.concatenate([kernel_ref[a, b, c] for a in range(3) for b in range(3)], axis=0)
            parts.append(jnp.dot(taps, weights, preferred_element_type=F32))
        left, here, right = parts
        if begin == 0:
            for t in range(step, frames):
                activate(t)
        blocks = []
        for n in range(step * rows):
            span = slice(n * width, (n + 1) * width)
            t, i = begin + n // rows, n % rows
            block = here[span] + shift_on(left[span]) + shift_back(right[span])
            second_ref[t, i] = block
            blocks.append(block)
        if begin == 0:
            total = sum(column_sum(b) for b in blocks)
            middle = group_sum(total) * (1.0 / (step * rows * width * (channels // GROUPS)))
            sums = total - middle * (step * rows * width)
            blocks = [second_ref[t, i] for t in range(step) for i in range(rows)]
            squares = sum(column_sum((b - middle) ** 2) for b in blocks)
        else:
            offs = [b - middle for b in blocks]
            sums = sums + sum(column_sum(off) for off in offs)
            squares = squares + sum(column_sum(off * off) for off in offs)
    store = pltpu.make_async_copy(
        rows_ref.at[cached + frames - 2 : cached + frames, 1 : 1 + rows], next_ref, sem
    )
    store.start()
    message_ref[...] = moments_row(middle, sums, squares, count)
    store.wait()


def final_kernel(second_ref, stats_ref, gain_ref, shift_ref, out_ref, buf, sems):
    frames, rows, width, channels = second_ref.shape
    members = frames * rows * width * (channels // GROUPS)
    center, factor = affine(unpack(stats_ref), members, gain_ref[...])
    offset = shift_ref[...]
    stores = []
    for t in range(frames):
        for i in range(rows):
            buf[t, i] = silu_norm(second_ref[t, i], center, factor, offset).astype(BF16)
            stores.append(pltpu.make_async_copy(buf.at[t, i], out_ref.at[t, i], sems.at[t * rows + i]))
            stores[-1].start()
    for c in stores:
        c.wait()


def both_kernel(mine_ref, other_ref, out_ref):
    both = jnp.concatenate([mine_ref[...], other_ref[...]], axis=1)
    out_ref[...] = jnp.broadcast_to(both[None], out_ref.shape)


def everyone(message):
    devices, chips = lax.axis_size(HA), lax.axis_size(HA[:-1])
    other = lax.ppermute(message, HA, [(i, i ^ 1) for i in range(devices)])
    copies = pl.pallas_call(
        both_kernel,
        name="both",
        out_shape=jax.ShapeDtypeStruct((chips, 1, 2 * LANES), F32),
        in_specs=[AUTO] * 2,
        out_specs=AUTO,
        compiler_params=limit(1),
    )(message, other)
    return lax.all_to_all(copies, HA[:-1], 0, 0)


def run_mix(row, last, above, below, ends, stats, gain, shift, hidden, kernel):
    frames, half, c_out = row.shape
    cached = hidden.shape[0]
    whole = jax.ShapeDtypeStruct
    return pl.pallas_call(
        mix_kernel,
        name="mix",
        out_shape=(
            whole((frames, 2, half, c_out), F32),
            whole((2, 2, half, c_out), BF16),
            whole((1, LANES), F32),
        ),
        in_specs=[AUTO] * 10,
        out_specs=(AUTO, ANY, AUTO),
        scratch_shapes=[pltpu.VMEM((cached + frames, 4, half, c_out), BF16), DMA(())],
        compiler_params=limit(28),
    )(row, last, above, below, ends, stats, gain, shift, hidden, kernel)


def local(video, cache_video, cache_hidden, kernel_down, gain_down, shift_down, kernel_mix, gain_mix, shift_mix):
    frames, rows, width, c_in = video.shape
    cached = cache_video.shape[0]
    c_out = kernel_down.shape[-1]
    half = width // 2
    video, cache_video, stored_hidden = (
        pltpu.with_memory_space_constraint(x, pltpu.HBM) for x in (video, cache_video, cache_hidden)
    )
    devices = lax.axis_size(HA)
    up = [((i + 1) % devices, i) for i in range(devices)]
    down = [(i, (i + 1) % devices) for i in range(devices)]
    whole = jax.ShapeDtypeStruct
    rim, ends = pl.pallas_call(
        rim_kernel,
        name="rim",
        out_shape=(whole((cached + frames, width, c_in), BF16), whole((3, c_out), F32)),
        in_specs=[HBM] * 2,
        out_specs=(AUTO,) * 2,
        scratch_shapes=[DMA((cached + frames,))],
        compiler_params=limit(4),
    )(cache_video, video)
    pairs = [(i, i ^ 1) for i in range(devices)]
    bridges = [(i, min(max(i + (1 if i % 2 else -1), 0), devices - 1)) for i in range(devices)]
    near_rim = lax.ppermute(rim, HA, pairs)
    far_rim = lax.ppermute(rim, HA, bridges)
    kernel_down = pltpu.with_memory_space_constraint(kernel_down, pltpu.HBM)
    line = whole((frames, half, c_out), F32)
    edge = whole((cached + 2 * frames, half, c_out), BF16)
    message = whole((1, LANES), F32)
    row, part, third, center, sums, below = pl.pallas_call(
        down_kernel,
        name="down",
        out_shape=(
            line,
            line,
            whole((3, 3, c_in, c_out), BF16),
            whole((1, c_out), F32),
            whole((2, c_out), F32),
            edge,
        ),
        in_specs=[HBM] * 4,
        out_specs=(AUTO,) * 6,
        scratch_shapes=[
            pltpu.VMEM(cache_video.shape, BF16),
            pltpu.VMEM(video.shape, BF16),
            pltpu.VMEM((3, 2, 3, c_in, c_out), BF16),
            pltpu.VMEM((cached + frames, rows, half, 2 * c_in), BF16),
            DMA((5,)),
        ],
        compiler_params=limit(24),
    )(cache_video, video, kernel_down, stored_hidden)
    below = lax.ppermute(below, HA, up)
    last, above, stats = pl.pallas_call(
        rim_down_kernel,
        name="rim_down",
        out_shape=(line, edge, message),
        in_specs=[AUTO] * 8,
        out_specs=(AUTO,) * 3,
        scratch_shapes=[
            pltpu.VMEM((cached + frames, width, c_in), BF16),
            pltpu.VMEM((cached + frames, half, 2 * c_in), BF16),
        ],
        compiler_params=limit(16),
    )(near_rim, far_rim, ends, third, part, center, sums, cache_hidden)
    above = lax.ppermute(above, HA, down)
    stats = everyone(stats)
    second, next_cache, stats = run_mix(
        row, last, above, below, ends, stats, gain_down[None], shift_down[None], cache_hidden, kernel_mix
    )
    stats = everyone(stats)
    encoded = pl.pallas_call(
        final_kernel,
        name="final",
        out_shape=whole((frames, 2, half, c_out), BF16),
        in_specs=[AUTO] * 4,
        out_specs=ANY,
        scratch_shapes=[pltpu.VMEM((frames, 2, half, c_out), BF16), DMA((2 * frames,))],
        compiler_params=limit(8),
    )(second, stats, gain_mix[None], shift_mix[None])
    return (encoded, next_cache)


def solution(mesh):
    split = Mesh(
        mesh.devices.reshape(mesh.shape["groups"], 8, 8, 2), ("groups", "ha_0", "ha_1", "ha_2")
    )
    strips = P("groups", HA, None, None)

    return jax.shard_map(
        local,
        mesh=split,
        in_specs=(strips, strips, strips, P(), P(), P(), P(), P(), P()),
        out_specs=(strips, strips),
        check_vma=False,
    )
```
